512 devices in a mesh: ctx: 128 (over x, z, core), kv: 4 (over y).
Axes of the slice: x: 4, y: 4, z: 16, core: 2. Of those that a mesh axis runs over, the one named last changes fastest.
Arguments:
- queries: bfloat16 [16384, 10752], P('ctx', 'kv'), may hold values from -64 to 64
- keys: bfloat16 [16384, 768], P('ctx', 'kv'), may hold values from -4 to 4
- values: bfloat16 [16384, 512], P('ctx', 'kv'), may hold values from -5 to 5
- key_weights: float32 [32, 768], P(None, 'kv'), may hold values from -1 to 1
- value_weights: float32 [32, 512], P(None, 'kv'), may hold values from -1 to 1
- picks: int32 [256, 16], P('ctx'), may hold values from -1 to 255, as said below
- gates: float32 [2, 16384, 56], P(None, 'ctx', 'kv'), may hold values from -6 to 6
Outputs:
- attended: bfloat16 [16384, 7168], P('ctx', 'kv')
The draws below stay inside these ranges and needn't reach their ends.
Inputs may be any that keep to these rules, and one draw needn't show every extreme that they name: `picks`: row t's first entry is t. Every other entry is -1 or a block p with p // 2 < t // 2. No row names a block twice, and the 2 rows t with the same t // 2 together name at most one block p for each value of p // 2 other than their own.
All inputs are finite; a program needn't handle non-finite values.
Results may differ from the reference program's by a relative error of at most 0.0061.
Values may be sent and summed in bfloat16 or wider, within the bound.
A program may use at most 64 MiB of HBM per device.

```python
import math
import jax
import jax.numpy as jnp
from jax import lax

HEADS = 56
GROUPS = 4
DQK = 192
DV = 128
BLOCK = 32
STRIDE = 16
TILE = 64
PICKS = 16
ROWS = 16384
TILES_DEV = 2
KEYBLOCKS = 256
CBLOCKS = 1024


def draw_pair(key):
    base = jax.random.fold_in(key, 7)
    key_rows = jax.random.normal(jax.random.fold_in(base, 1), (ROWS, GROUPS, DQK), jnp.float32)
    query_rows = jax.random.normal(jax.random.fold_in(base, 2), (ROWS, HEADS, DQK), jnp.float32)
    key_rows = jnp.clip(key_rows, -4.0, 4.0)
    query_rows = jnp.clip(query_rows, -64.0, 64.0)
    return (query_rows.reshape(ROWS, HEADS * DQK), key_rows.reshape(ROWS, GROUPS * DQK))


def draw_queries(key, part):
    return draw_pair(key)[0].astype(jnp.bfloat16)


def draw_keys(key, part):
    return draw_pair(key)[1].astype(jnp.bfloat16)


def draw_picks(key, part):
    shards = KEYBLOCKS // TILES_DEV
    device = jnp.arange(shards, dtype=jnp.int32)[:, None]
    owners = jnp.arange(shards, dtype=jnp.int32)[None, :]
    noise = jax.random.randint(jax.random.fold_in(key, 11), (shards, shards), 0, 1 << 20)
    ranked = jnp.where(owners < device, noise, 1 << 21) * shards + owners
    listed = jnp.argsort(ranked, axis=1, stable=True).astype(jnp.int32)
    slot = jnp.arange(TILES_DEV, dtype=jnp.int32)[:, None] * (PICKS - 1) + jnp.arange(PICKS - 1, dtype=jnp.int32)[None, :]
    clipped = jnp.minimum(slot, shards - 1)
    chosen = listed[:, clipped]
    within = jax.random.randint(jax.random.fold_in(key, 12), (shards, TILES_DEV, PICKS - 1), 0, TILES_DEV)
    usable = slot[None, :, :] < device[:, :, None]
    remote = jnp.where(usable, chosen * TILES_DEV + within, -1)
    own = device[:, :, None] * TILES_DEV + jnp.arange(TILES_DEV, dtype=jnp.int32)[None, :, None]
    return jnp.concatenate([own, remote], 2).reshape(KEYBLOCKS, PICKS).astype(jnp.int32)


def block_scale(stream_key, extent, cuts, smallest, largest):
    gain, own = 1.0, jax.random.fold_in(stream_key, 6)
    for dim, shards_of in cuts:
        steps = jnp.exp(jax.random.uniform(jax.random.fold_in(own, dim), (shards_of,), jnp.float32, smallest / len(cuts), largest / len(cuts)))
        gain = gain * jnp.repeat(steps, extent[dim] // shards_of).reshape([-1 if axis == dim else 1 for axis in range(len(extent))])
    return gain


def gaussian(stream_key, dims, spread, most, cuts=(), kind=jnp.bfloat16):
    result = jax.random.normal(stream_key, dims, jnp.float32) * spread
    if len(cuts) > 0:
        result = block_scale(stream_key, dims, cuts, -0.22, 0.18) * result
    return jnp.clip(result, min=-most, max=most).astype(kind)


def setup_inputs(seed: int = 0) -> dict:
    key_of = jax.random.split(jax.random.key(seed), 8)
    queries = draw_queries(jax.random.fold_in(key_of[7], 71), 0)
    keys = draw_keys(jax.random.fold_in(key_of[7], 71), 0)
    values = gaussian(key_of[2], (ROWS, GROUPS * DV), 1.0, 5.0, ((0, 128), (1, 4)))
    key_weights = gaussian(key_of[3], (BLOCK, GROUPS * DQK), BLOCK ** -0.5, 1.0, ((1, 4),), jnp.float32)
    value_weights = gaussian(key_of[4], (BLOCK, GROUPS * DV), BLOCK ** -0.5, 1.0, ((1, 4),), jnp.float32)
    picks = draw_picks(jax.random.fold_in(key_of[7], 71), 0)
    gates = gaussian(key_of[6], (2, ROWS, HEADS), 1.5, 6.0, ((1, 128), (2, 4)), jnp.float32)
    return {"queries": queries, "keys": keys, "values": values, "key_weights": key_weights, "value_weights": value_weights, "picks": picks, "gates": gates}


neg_large = -1e+30

def compress(rows_in, weights):
    count = rows_in.shape[0]
    width = rows_in.shape[1]
    joined = jnp.concatenate([rows_in.astype(jnp.float32), jnp.zeros((STRIDE, width), jnp.float32)], 0)
    starts = joined[:count].reshape(count // STRIDE, STRIDE, width)
    ends = joined[STRIDE:].reshape(count // STRIDE, STRIDE, width)
    both = jnp.concatenate([starts, ends], 1)
    mixed = jnp.einsum('bjd,jd->bd', both, weights.astype(jnp.float32), precision=lax.Precision.HIGHEST)
    return mixed.astype(jnp.bfloat16)

def reference(queries, keys, values, key_weights, value_weights, picks, gates):
    per_group = HEADS // GROUPS
    inv_root = 1.0 / math.sqrt(DQK)
    query_all = queries.reshape(ROWS, GROUPS, per_group, DQK)
    gating = jax.nn.sigmoid(gates.astype(jnp.float32))
    span = min(512, ROWS)
    block_end = jnp.arange(CBLOCKS, dtype=jnp.int32) * STRIDE + BLOCK - 1
    results = []
    for group in range(GROUPS):
        group_keys = keys[:, group * DQK:(group + 1) * DQK]
        group_values = values[:, group * DV:(group + 1) * DV]
        comp_keys = compress(group_keys, key_weights[:, group * DQK:(group + 1) * DQK]).astype(jnp.float32)
        comp_values = compress(group_values, value_weights[:, group * DV:(group + 1) * DV]).astype(jnp.float32)
        group_queries = query_all[:, group]

        def compressed_part(offset):
            batch = lax.dynamic_slice_in_dim(group_queries, offset, span, 0).astype(jnp.float32)
            scores = jnp.einsum('rhd,bd->rhb', batch, comp_keys) * inv_root
            position = offset + jnp.arange(span, dtype=jnp.int32)
            visible = (block_end[None, :] <= position[:, None])[:, None, :]
            top_score = lax.optimization_barrier(jnp.max(jnp.where(visible, scores, neg_large), axis=2, keepdims=True))
            weights = jnp.where(visible, jnp.exp(scores - top_score), 0.0)
            mass_sum = lax.optimization_barrier(jnp.sum(weights, axis=2))
            summed = jnp.einsum('rhb,bd->rhd', weights.astype(jnp.bfloat16).astype(jnp.float32), comp_values)
            return summed / jnp.maximum(mass_sum, 1.0)[..., None]
        offsets = jnp.arange(ROWS // span, dtype=jnp.int32) * span
        comp_out = lax.map(compressed_part, offsets).reshape(ROWS, per_group, DV)
        key_table = group_keys.reshape(KEYBLOCKS, TILE, DQK)
        value_table = group_values.reshape(KEYBLOCKS, TILE, DV)

        def selected_part(tile_index):
            picked = picks[tile_index]
            safe = jnp.maximum(picked, 0).astype(jnp.int32)
            chosen_keys = key_table[safe].reshape(PICKS * TILE, DQK).astype(jnp.float32)
            chosen_values = value_table[safe].reshape(PICKS * TILE, DV).astype(jnp.float32)
            start_row = (tile_index * TILE).astype(jnp.int32)
            batch = lax.dynamic_slice_in_dim(group_queries, start_row, TILE, 0).astype(jnp.float32)
            scores = jnp.einsum('rhd,kd->rhk', batch, chosen_keys) * inv_root
            position = start_row + jnp.arange(TILE, dtype=jnp.int32)
            key_pos = (safe[:, None] * TILE + jnp.arange(TILE, dtype=jnp.int32)[None, :]).reshape(-1)
            live = jnp.repeat(picked >= 0, TILE)
            visible = (live[None, :] & (key_pos[None, :] <= position[:, None]))[:, None, :]
            top_score = lax.optimization_barrier(jnp.max(jnp.where(visible, scores, neg_large), axis=2, keepdims=True))
            weights = jnp.where(visible, jnp.exp(scores - top_score), 0.0)
            mass_sum = lax.optimization_barrier(jnp.sum(weights, axis=2))
            summed = jnp.einsum('rhk,kd->rhd', weights.astype(jnp.bfloat16).astype(jnp.float32), chosen_values)
            return summed / mass_sum[..., None]
        sel_out = lax.map(selected_part, jnp.arange(KEYBLOCKS, dtype=jnp.int32)).reshape(ROWS, per_group, DV)
        head_slice = slice(group * per_group, (group + 1) * per_group)
        mixed = gating[0][:, head_slice][..., None] * comp_out + gating[1][:, head_slice][..., None] * sel_out
        results.append(mixed)
    stacked = jnp.stack(results, 1).reshape(ROWS, HEADS * DV)
    return stacked.astype(jnp.bfloat16)
```

```python
import jax
import jax.numpy as jnp
from jax import lax
from jax.experimental import pallas as pl
from jax.experimental.pallas import tpu as pltpu
from jax.sharding import PartitionSpec as P

NX = 4
NZ = 16
HEADS = 14
PAIRS = HEADS // 2
DQK = 192
DV = 128
ROWS = 128
TILE = 64
PICKS = 16
CROWS = 32
KROWS = DQK + CROWS
LOW = -1e30
FLOOR = -1e29
COEF = DQK ** (-0.5) * 1.4426950408889634
F32 = jnp.float32
BF16 = jnp.bfloat16
MESH = pl.DeviceIdType.MESH


def gather_body(
    q_any, k_ref, v_ref, kw_ref, vw_ref, kb, vb, o_sc,
    q_vm, halo_k, halo_v, m_sc, cvext,
    q_sem, halo_s, halo_r, zk_s, zk_r, zv_s, zv_r, xv_s, xv_r, xk_s, xk_r, pk_s, pk_r, pv_s, pv_r,
):
    i = lax.axis_index("ctx")
    x = i // 32
    z = (i // 2) % NZ
    c = i % 2

    def at(xx, zz, cc):
        return (xx % NX) * 32 + (zz % NZ) * 2 + cc

    zside = (at(x, z + 1, c), at(x, z + NZ - 1, c))
    xside = (at(x + 1, z, c), at(x + NX - 1, z, c))
    partner = at(x, z, 1 - c)
    before = (i + 127) % 128
    after = (i + 1) % 128
    sends = []

    def remote(src, dst, ss, rs, target):
        return pltpu.make_async_remote_copy(
            src_ref=src, dst_ref=dst, send_sem=ss, recv_sem=rs,
            device_id={"ctx": target}, device_id_type=MESH,
        )

    def send(ref, ss, rs, target, dst=None):
        copy = remote(ref, ref if dst is None else dst, ss, rs, target)
        copy.start()
        sends.append(copy)

    def arrived(ref, ss, rs):
        remote(ref, ref, ss, rs, partner).wait_recv()

    barrier = pltpu.get_barrier_semaphore()
    for peer in (*zside, *xside, partner, before, after):
        pl.semaphore_signal(barrier, inc=1, device_id={"ctx": peer}, device_id_type=MESH)
    q_copy = pltpu.make_async_copy(q_any, q_vm, q_sem)
    q_copy.start()

    keys = k_ref[...].astype(F32)
    own_k = kb.at[c, z, x]
    own_k[pl.ds(0, 128), :] = jnp.transpose(keys[:, :128]).astype(BF16)
    own_k[pl.ds(128, 64), :] = jnp.transpose(keys[:, 128:]).astype(BF16)
    vb[c, z, x] = v_ref[...]
    pl.semaphore_wait(barrier, 7)

    send(k_ref.at[pl.ds(0, 16), :], halo_s.at[0], halo_r.at[0], before, halo_k)
    send(v_ref.at[pl.ds(0, 16), :], halo_s.at[1], halo_r.at[1], before, halo_v)

    def vz_send(zz, xx, step, col, dirs=(0, 1)):
        for d in dirs:
            send(vb.at[c, zz, xx], zv_s.at[d, step, col], zv_r.at[d, step, col], zside[d])

    for d in range(2):
        send(vb.at[c, z, x], xv_s.at[d], xv_r.at[d], xside[d])
    vz_send(z, x, 1, 0)

    o_sc[...] = jnp.zeros_like(o_sc)
    m_sc[...] = jnp.full_like(m_sc, FLOOR)
    cvext[:, 128:] = jnp.ones((128, 128), BF16)

    arrived(halo_k, halo_s.at[0], halo_r.at[0])
    arrived(halo_v, halo_s.at[1], halo_r.at[1])
    inside = (i != 127).astype(F32)

    def compress(rows, extra, weights):
        joined = jnp.concatenate([rows, extra.astype(F32) * inside], 0)
        parts = [
            jnp.sum(joined[16 * b:16 * b + 32] * weights, axis=0, keepdims=True) for b in range(8)
        ]
        return jnp.concatenate(parts, 0)

    ck = compress(keys, halo_k[...], kw_ref[...])
    cv = compress(v_ref[...].astype(F32), halo_v[...], vw_ref[...])
    zeros64 = jnp.zeros((8, 64), F32)
    ck_low = jnp.concatenate([ck[:, 128:], zeros64], 1)
    own_k[pl.ds(192, 16), :] = jnp.concatenate([ck[:, :128], ck_low], 0).astype(BF16)
    own_k[pl.ds(208, 16), :] = jnp.concatenate([cv, jnp.zeros((8, 128), F32)], 0).astype(BF16)

    def kx_send(zz):
        for d in range(2):
            send(kb.at[c, zz, x], xk_s.at[zz, d], xk_r.at[zz, d], xside[d])

    for d in range(2):
        send(kb.at[c, z, x], zk_s.at[d, 1], zk_r.at[d, 1], zside[d])
    kx_send(z)

    xm, xp, xo = (x + 3) % NX, (x + 1) % NX, (x + 2) % NX
    cols = (x, xm, xp, xo)
    arrived(vb.at[c, z, xm], xv_s.at[0], xv_r.at[0])
    top = vb.at[c, z, xm, pl.ds(0, 64), :]
    send(top, xv_s.at[2], xv_r.at[2], xside[0])
    vz_send(z, xm, 1, 1)
    arrived(vb.at[c, z, xp], xv_s.at[1], xv_r.at[1])
    low = vb.at[c, z, xp, pl.ds(64, 64), :]
    send(low, xv_s.at[3], xv_r.at[3], xside[1])
    vz_send(z, xp, 1, 2)
    arrived(vb.at[c, z, xo, pl.ds(0, 64), :], xv_s.at[2], xv_r.at[2])
    arrived(vb.at[c, z, xo, pl.ds(64, 64), :], xv_s.at[3], xv_r.at[3])
    vz_send(z, xo, 1, 3)
    q_copy.wait()

    row_of = i * ROWS + lax.broadcasted_iota(jnp.int32, (ROWS, 128), 0)
    lane = lax.broadcasted_iota(jnp.int32, (ROWS, 128), 1)

    def flash(za, zb):
        ck0, ck1, cvs = [], [], []
        for zz in (za, zb):
            for xx in range(NX):
                for cc in range(2):
                    first = kb[cc, zz, xx, pl.ds(192, 16), :].astype(F32)
                    second = kb[cc, zz, xx, pl.ds(208, 16), :].astype(F32)
                    ck0.append(first[:8])
                    ck1.append(first[8:])
                    cvs.append(second[:8])
        ck0 = jnp.concatenate(ck0, 0)
        ck1 = jnp.concatenate(ck1, 0)
        cvext[:, :128] = jnp.concatenate(cvs, 0).astype(BF16)
        even = jnp.concatenate([ck0, ck1], 1).astype(BF16)
        r0 = pltpu.roll(ck0, 64, 1)
        r1 = pltpu.roll(ck1, 64, 1)
        odd = jnp.concatenate(
            [jnp.where(lane < 64, r1, r0), jnp.where(lane < 64, r0, r1)], 1
        ).astype(BF16)
        zed = jnp.where(lane < 64, za, zb)
        block = (((lane // 16) % 4) * 32 + zed * 2 + (lane // 8) % 2) * 8 + lane % 8
        bias = jnp.where(block * 16 + 31 <= row_of, 0.0, LOW).astype(F32)
        extended = cvext[...]

        def pair(p, carry):
            two = q_vm[:, pl.ds(pl.multiple_of(p * 384, 128), 384)]
            for par, table in ((0, even), (1, odd)):
                h = 2 * p + par
                score = lax.dot_general(
                    two[:, 128 * par:128 * par + 256], table, (((1,), (1,)), ((), ())),
                    preferred_element_type=F32,
                ) + bias
                old = m_sc[h]
                new = jnp.maximum(old, jnp.max(score, axis=1, keepdims=True))
                weight = jnp.exp2((score - new) * COEF)
                scale = jnp.exp2((old - new) * COEF)
                m_sc[h] = new
                added = jnp.dot(weight.astype(BF16), extended, preferred_element_type=F32)
                o_sc[h] = o_sc[h] * jnp.concatenate([scale, scale], 1) + added
            return carry

        lax.fori_loop(0, PAIRS, pair, 0)

    def sources(step):
        if step == 0:
            return (z,)
        if step == 8:
            return ((z + 8) % NZ,)
        return ((z + NZ - step) % NZ, (z + step) % NZ)

    half = KROWS // 2
    for step in range(1, 12):
        if step <= 7:
            src = sources(step)
            for d in range(2):
                chunk = kb.at[c, src[d], x]
                arrived(chunk, zk_s.at[d, step], zk_r.at[d, step])
                if step < 7:
                    send(chunk, zk_s.at[d, step + 1], zk_r.at[d, step + 1], zside[d])
                else:
                    piece = kb.at[c, src[d], x, pl.ds(d * half, half), :]
                    send(piece, zk_s.at[d, 8], zk_r.at[d, 8], zside[d])
                kx_send(src[d])
            for col in range(4):
                for d in range(2):
                    arrived(vb.at[c, src[d], cols[col]], zv_s.at[d, step, col], zv_r.at[d, step, col])
                    if step < 7 or (col % 2) == d:
                        vz_send(src[d], cols[col], step + 1, col, (d,))
        if step == 8:
            far = sources(8)[0]
            for d in range(2):
                piece = kb.at[c, far, x, pl.ds(d * half, half), :]
                arrived(piece, zk_s.at[d, 8], zk_r.at[d, 8])
            kx_send(far)
            for col in range(4):
                d = col % 2
                arrived(vb.at[c, far, cols[col]], zv_s.at[d, 8, col], zv_r.at[d, 8, col])
        if 0 <= step - 1 <= 8:
            for zz in sources(step - 1):
                arrived(kb.at[c, zz, xm], xk_s.at[zz, 0], xk_r.at[zz, 0])
                arrived(kb.at[c, zz, xp], xk_s.at[zz, 1], xk_r.at[zz, 1])
                sign = 1 - 2 * (zz % 2)
                origin = (x + NX - sign) % NX
                send(
                    kb.at[c, zz, origin], xk_s.at[zz, 2], xk_r.at[zz, 2], at(x + NX + sign, z, c)
                )
        if 0 <= step - 2 <= 8:
            for zz in sources(step - 2):
                arrived(kb.at[c, zz, xo], xk_s.at[zz, 2], xk_r.at[zz, 2])
                send(kb.at[c, zz], pk_s.at[zz], pk_r.at[zz], partner)
                send(vb.at[c, zz], pv_s.at[zz], pv_r.at[zz], partner)
        if 0 <= step - 3 <= 8:
            for zz in sources(step - 3):
                arrived(kb.at[1 - c, zz], pk_s.at[zz], pk_r.at[zz])
                arrived(vb.at[1 - c, zz], pv_s.at[zz], pv_r.at[zz])
            if 1 <= step - 3 <= 7:
                flash(*sources(step - 3))
    flash(z, sources(8)[0])

    for copy in sends:
        copy.wait_send()


def select_body(q_vm, kb, vb, o_sc, picks_ref, g_ref, out_ref, s_sc, p_sc, ks, vext):
    i = lax.axis_index("ctx")
    vext[:, 128:] = jnp.ones((1024, 128), BF16)
    ks[0:64, :] = jnp.zeros((64, 1024), BF16)
    ks[256:320, :] = jnp.zeros((64, 1024), BF16)
    gate = jax.nn.sigmoid(g_ref[...])
    half_lane = lax.broadcasted_iota(jnp.int32, (DQK, 128), 1)
    small_lane = lax.broadcasted_iota(jnp.int32, (TILE, 128), 1)
    small_row = lax.broadcasted_iota(jnp.int32, (TILE, 128), 0)
    for t in range(2):
        biases = []
        for j in range(PICKS // 2):
            tiles, sides, shifts = [], [], []
            for e in range(2):
                pick = picks_ref[t, 2 * j + e]
                safe = jnp.where(pick < 0, 2 * i + t, pick)
                owner = safe // 2
                part = safe % 2
                ox, oz, oc = owner // 32, (owner // 2) % NZ, owner % 2
                tile = kb[oc, oz, ox, pl.ds(0, DQK), :].astype(F32)
                shift = part * 64 if e == 0 else (1 - part) * 64
                tiles.append(pltpu.roll(tile, shift, 1))
                start = pl.multiple_of(part * 64, 64)
                vext[128 * j + 64 * e:128 * j + 64 * e + 64, :128] = vb[oc, oz, ox, pl.ds(start, 64), :]
                sides.append(jnp.where(pick < 0, LOW, 0.0).astype(F32))
            ks[64:256, 128 * j:128 * j + 128] = jnp.where(half_lane < 64, tiles[0], tiles[1]).astype(BF16)
            bias = jnp.where(small_lane < 64, sides[0], sides[1])
            if j == 0:
                bias = jnp.where((small_lane < 64) & (small_lane > small_row), LOW, bias)
            biases.append(bias)
        for par in range(2):
            rows = jnp.concatenate(
                [
                    q_vm[64 * t:64 * t + 64, 384 * p + 128 * par:384 * p + 128 * par + 256]
                    for p in range(PAIRS)
                ],
                0,
            )
            table = ks[64 - 64 * par:320 - 64 * par, :]
            s_sc[...] = jnp.dot(rows, table, preferred_element_type=F32)
            for p in range(PAIRS):
                pieces = [
                    s_sc[64 * p:64 * p + 64, 128 * j:128 * j + 128] + biases[j]
                    for j in range(PICKS // 2)
                ]
                score = jnp.concatenate(pieces, 1)
                top_score = jnp.max(score, axis=1, keepdims=True)
                p_sc[64 * p:64 * p + 64, :] = jnp.exp2((score - top_score) * COEF).astype(BF16)
            result = jnp.dot(p_sc[...], vext[...], preferred_element_type=F32)
            for p in range(PAIRS):
                h = 2 * p + par
                rs = slice(64 * t, 64 * t + 64)
                sel = result[64 * p:64 * p + 64, :128] / result[64 * p:64 * p + 64, 128:]
                comp = o_sc[h, rs, :128] / jnp.maximum(o_sc[h, rs, 128:], 1.0)
                mixed = gate[0, rs, h:h + 1] * comp + gate[1, rs, h:h + 1] * sel
                out_ref[rs, h * DV:(h + 1) * DV] = mixed.astype(BF16)


def local(queries, keys, values, key_weights, value_weights, picks, gates):
    vmem = pl.BlockSpec(memory_space=pltpu.VMEM)
    dma = pltpu.SemaphoreType.DMA
    kb, vb, comp = pl.pallas_call(
        gather_body,
        out_shape=[
            pltpu.VMEM((2, NZ, NX, KROWS, 128), BF16),
            pltpu.VMEM((2, NZ, NX, ROWS, 128), BF16),
            pltpu.VMEM((HEADS, ROWS, 256), F32),
        ],
        in_specs=[pl.BlockSpec(memory_space=pl.ANY), vmem, vmem, vmem, vmem],
        out_specs=[vmem, vmem, vmem],
        scratch_shapes=[
            pltpu.VMEM((ROWS, HEADS * DQK), BF16),
            pltpu.VMEM((16, DQK), BF16),
            pltpu.VMEM((16, DV), BF16),
            pltpu.VMEM((HEADS, ROWS, 128), F32),
            pltpu.VMEM((128, 256), BF16),
            dma,
            dma((2,)), dma((2,)),
            dma((2, 9)), dma((2, 9)),
            dma((2, 9, 4)), dma((2, 9, 4)),
            dma((4,)), dma((4,)),
            dma((NZ, 3)), dma((NZ, 3)),
            dma((NZ,)), dma((NZ,)),
            dma((NZ,)), dma((NZ,)),
        ],
        compiler_params=pltpu.CompilerParams(
            collective_id=0, has_side_effects=True, vmem_limit_bytes=32 * 1024 * 1024
        ),
        name="gather_compressed",
    )(queries, keys, values, key_weights, value_weights)
    return pl.pallas_call(
        select_body,
        out_shape=jax.ShapeDtypeStruct((ROWS, HEADS * DV), BF16),
        in_specs=[vmem, vmem, vmem, vmem, pl.BlockSpec(memory_space=pltpu.SMEM), vmem],
        out_specs=vmem,
        scratch_shapes=[
            pltpu.VMEM((PAIRS * TILE, 1024), F32),
            pltpu.VMEM((PAIRS * TILE, 1024), BF16),
            pltpu.VMEM((320, 1024), BF16),
            pltpu.VMEM((1024, 256), BF16),
        ],
        compiler_params=pltpu.CompilerParams(vmem_limit_bytes=32 * 1024 * 1024),
        name="selected_mix",
    )(queries, kb, vb, comp, picks, gates)


def solution(mesh):
    in_specs = (
        P("ctx", "kv"), P("ctx", "kv"), P("ctx", "kv"), P(None, "kv"), P(None, "kv"),
        P("ctx", None), P(None, "ctx", "kv"),
    )
    return jax.shard_map(
        local, mesh=mesh, in_specs=in_specs, out_specs=P("ctx", "kv"), check_vma=False
    )
```

```python
import jax
import jax.numpy as jnp
from jax import lax
from jax.experimental import pallas as pl
from jax.experimental.pallas import tpu as pltpu
from jax.sharding import PartitionSpec as P

NX = 4
NZ = 16
HEADS = 14
PAIRS = HEADS // 2
DQK = 192
DV = 128
ROWS = 128
TILE = 64
PICKS = 16
CROWS = 48
KROWS = 2 * DQK + CROWS
LOW = -1e30
FLOOR = -1e29
COEF = DQK ** (-0.5) * 1.4426950408889634
F32 = jnp.float32
BF16 = jnp.bfloat16
MESH = pl.DeviceIdType.MESH


def guard(cond, step):
    if isinstance(cond, bool):
        if cond:
            step()
    else:
        pl.when(cond)(step)


def gather_body(
    q_any, kt_any, v_any, kw_any, vw_any, g_any,
    kb, vb, q_vm, gate_out,
    kw, vw, g_vm, halo_src, halo_k, halo_v,
    in_s, halo_s, halo_r, ex_s, ex_r, zk_s, zk_r, zv_s, zv_r, xv_s, xv_r, xk_s, xk_r,
    pk_s, pk_r, pv_s, pv_r,
):
    i = lax.axis_index("ctx")
    x = i // 32
    z = (i // 2) % NZ
    c = i % 2

    def at(xx, zz, cc):
        return (xx % NX) * 32 + (zz % NZ) * 2 + cc

    zside = (at(x, z + 1, c), at(x, z + NZ - 1, c))
    xside = (at(x + 1, z, c), at(x + NX - 1, z, c))
    partner = at(x, z, 1 - c)
    before = (i + 127) % 128
    after = (i + 1) % 128
    xm, xp, xo = (x + 3) % NX, (x + 1) % NX, (x + 2) % NX
    cols = (x, xm, xp, xo)

    def remote(src, dst, ss, rs, target):
        return pltpu.make_async_remote_copy(
            src_ref=src, dst_ref=dst, send_sem=ss, recv_sem=rs,
            device_id={"ctx": target}, device_id_type=MESH,
        )

    def send(ref, ss, rs, target, dst=None):
        remote(ref, ref if dst is None else dst, ss, rs, target).start()

    def arrived(ref, ss, rs):
        remote(ref, ref, ss, rs, partner).wait_recv()

    def left(ref, ss, rs):
        remote(ref, ref, ss, rs, partner).wait_send()

    barrier = pltpu.get_barrier_semaphore()
    for peer in (*zside, *xside, partner, before, after):
        pl.semaphore_signal(barrier, inc=1, device_id={"ctx": peer}, device_id_type=MESH)
    own_k = kb.at[z, x, pl.ds(pl.multiple_of(c * DQK, 64), DQK), :]
    own_v = vb.at[z, x, c]
    loads = [
        pltpu.make_async_copy(src, dst, in_s.at[n])
        for n, (src, dst) in enumerate([
            (kt_any, own_k), (v_any, own_v), (kw_any, kw), (vw_any, vw), (g_any, g_vm),
            (q_any, q_vm),
        ])
    ]
    for load in loads:
        load.start()
    loads[0].wait()
    loads[1].wait()
    first = jnp.transpose(own_k[pl.ds(0, 128), :].astype(F32))
    second = jnp.transpose(own_k[pl.ds(128, 64), :].astype(F32))
    halo_src[...] = jnp.concatenate([first[:16], second[:16]], 1).astype(BF16)
    pl.semaphore_wait(barrier, 7)

    send(own_k, ex_s.at[0], ex_r.at[0], partner)
    send(own_v, ex_s.at[1], ex_r.at[1], partner)

    @pl.when(c == 0)
    def _():
        send(halo_src, halo_s.at[0], halo_r.at[0], before, halo_k)
        send(own_v.at[pl.ds(0, 16), :], halo_s.at[1], halo_r.at[1], before, halo_v)

    own_keys = [kb.at[z, col] for col in cols[1:]] + [kb.at[z, x, pl.ds(2 * DQK, CROWS), :]]
    own_values = [vb.at[z, col] for col in cols[1:]]

    def pull(step, d):
        return (z + NZ - step) % NZ if d == 0 else (z + step) % NZ

    @pl.when(c == 1)
    def _():
        spans = (pl.ds(0, DQK), pl.ds(DQK, DQK), pl.ds(2 * DQK, CROWS))
        wide = (pl.ds(0, DQK), pl.ds(DQK, DQK + CROWS))
        late = (0, 1, 1)

        def kz_send(zz, step, piece, d):
            part = kb.at[zz, x, spans[piece], :]
            send(part, zk_s.at[d, step, piece], zk_r.at[d, step, piece], zside[d])

        def kz_wait(zz, step, piece, d):
            part = kb.at[zz, x, spans[piece], :]
            arrived(part, zk_s.at[d, step, piece], zk_r.at[d, step, piece])

        def kx_send(zz, w):
            for d in range(2):
                send(kb.at[zz, x, wide[w], :], xk_s.at[zz, d, w], xk_r.at[zz, d, w], xside[d])

        def both(q, run):
            if isinstance(q, int):
                guard(q >= 0, lambda: run(pull(q, 0)))
                guard(0 < q < 8, lambda: run(pull(q, 1)))
            else:
                guard(q >= 0, lambda: run(pull(q, 0)))
                guard(q > 0, lambda: run(pull(q, 1)))

        def x_step(q, w):
            def move(zz):
                for d, col in ((0, xm), (1, xp)):
                    arrived(kb.at[zz, col, wide[w], :], xk_s.at[zz, d, w], xk_r.at[zz, d, w])
                sign = 1 - 2 * (zz % 2)
                origin = (x + NX - sign) % NX
                send(
                    kb.at[zz, origin, wide[w], :], xk_s.at[zz, 2, w], xk_r.at[zz, 2, w],
                    at(x + NX + sign, z, c),
                )

            both(q, move)

        def p_step(q):
            def landed(zz):
                for w in range(2):
                    arrived(kb.at[zz, xo, wide[w], :], xk_s.at[zz, 2, w], xk_r.at[zz, 2, w])

            def move(zz):
                landed(zz)
                send(kb.at[zz], pk_s.at[zz], pk_r.at[zz], partner)

            def move_own():
                landed(z)
                for n, part in enumerate(own_keys):
                    send(part, pk_s.at[NZ + n], pk_r.at[NZ + n], partner)

            if isinstance(q, int):
                guard(q > 0, lambda: move(pull(q, 0)))
                guard(0 < q < 8, lambda: move(pull(q, 1)))
            else:
                guard(q > 0, lambda: (move(pull(q, 0)), move(pull(q, 1)))[0])
            guard(q == 0, move_own)

        for d in range(2):
            kz_send(z, 1, 1, d)
        arrived(kb.at[z, x, spans[0], :], ex_s.at[0], ex_r.at[0])
        for d in range(2):
            kz_send(z, 1, 0, d)
        kx_send(z, 0)
        arrived(vb.at[z, x, 0], ex_s.at[1], ex_r.at[1])
        loads[2].wait()
        loads[3].wait()
        other = kb[z, x, pl.ds(0, DQK), :].astype(F32)
        natural = jnp.concatenate(
            [
                jnp.concatenate([jnp.transpose(other[:128]), jnp.transpose(other[128:])], 1),
                jnp.concatenate([first, second], 1),
            ],
            0,
        )
        chip_v = jnp.concatenate([vb[z, x, 0], vb[z, x, 1]], 0).astype(F32)
        arrived(halo_k, halo_s.at[0], halo_r.at[0])
        arrived(halo_v, halo_s.at[1], halo_r.at[1])
        inside = (i != 127).astype(F32)

        def compress(rows, extra, weights):
            joined = jnp.concatenate([rows, extra.astype(F32) * inside], 0)
            parts = [
                jnp.sum(joined[16 * b:16 * b + 32] * weights, axis=0, keepdims=True)
                for b in range(16)
            ]
            return jnp.concatenate(parts, 0)

        ck = compress(natural, halo_k[...], kw[...])
        cv = compress(chip_v, halo_v[...], vw[...])
        own = kb.at[z, x]
        own[pl.ds(2 * DQK, 16), :] = ck[:, :128].astype(BF16)
        own[pl.ds(2 * DQK + 16, 16), :] = jnp.concatenate(
            [ck[:, 128:], jnp.zeros((16, 64), F32)], 1
        ).astype(BF16)
        own[pl.ds(2 * DQK + 32, 16), :] = cv.astype(BF16)
        for d in range(2):
            kz_send(z, 1, 2, d)
        kx_send(z, 1)
        loads[5].wait()

        def z_step(s, piece, forward):
            for d in range(2):
                zz = pull(s, d)
                kz_wait(zz, s, piece, d)
                if forward or late[piece] == d:
                    kz_send(zz, s + 1, piece, d)
                if piece != 1:
                    kx_send(zz, late[piece])

        def round_of(s, forward):
            z_step(s, 0, forward)
            z_step(s, 1, forward)
            x_step(s - 1, 0)
            z_step(s, 2, forward)
            x_step(s - 2, 1)
            p_step(s - 3)

        def loop_round(s, carry):
            round_of(s, True)
            return carry

        lax.fori_loop(1, 7, loop_round, 0)
        round_of(7, False)
        far = (z + 8) % NZ
        kz_wait(far, 8, 0, 0)
        kx_send(far, 0)
        x_step(7, 0)
        x_step(6, 1)
        kz_wait(far, 8, 1, 1)
        kz_wait(far, 8, 2, 1)
        kx_send(far, 1)
        x_step(8, 0)
        p_step(5)
        x_step(7, 1)
        p_step(6)
        x_step(8, 1)
        p_step(7)
        p_step(8)
        loads[4].wait()
        columns = jnp.concatenate(
            [g_vm[h] for h in range(HEADS)] + [jnp.zeros((4, ROWS), F32)], 0
        )
        gate_out[...] = jax.nn.sigmoid(jnp.transpose(columns))

        for zz in range(NZ):
            for d in range(3):
                for w in range(2):
                    left(kb.at[zz, x, wide[w], :], xk_s.at[zz, d, w], xk_r.at[zz, d, w])
        for k in range(1, NZ):
            zz = (z + k) % NZ
            left(kb.at[zz], pk_s.at[zz], pk_r.at[zz])
        for n, part in enumerate(own_keys):
            left(part, pk_s.at[NZ + n], pk_r.at[NZ + n])
        for s in range(1, 9):
            for piece in range(3):
                for d in range(2):
                    if s < 8 or late[piece] == d:
                        part = kb.at[z, x, spans[piece], :]
                        left(part, zk_s.at[d, s, piece], zk_r.at[d, s, piece])
        for k in range(1, NZ):
            zz = (z + k) % NZ
            arrived(vb.at[zz], pv_s.at[zz], pv_r.at[zz])
        for n, part in enumerate(own_values):
            arrived(part, pv_s.at[NZ + n], pv_r.at[NZ + n])
        left(own_k, ex_s.at[0], ex_r.at[0])
        left(own_v, ex_s.at[1], ex_r.at[1])

    @pl.when(c == 0)
    def _():
        def vz_send(zz, xx, step, col, d):
            send(vb.at[zz, xx], zv_s.at[d, step, col], zv_r.at[d, step, col], zside[d])

        def vz_wait(zz, xx, step, col, d):
            arrived(vb.at[zz, xx], zv_s.at[d, step, col], zv_r.at[d, step, col])

        def p_send(zz):
            send(vb.at[zz], pv_s.at[zz], pv_r.at[zz], partner)

        def k_wait(q):
            for d in range(2):
                zz = pull(q, d)

                def hold(zz=zz):
                    arrived(kb.at[zz], pk_s.at[zz], pk_r.at[zz])

                guard(q > 0 if d == 0 or not isinstance(q, int) else 0 < q < 8, hold)

            def hold_own():
                for n, part in enumerate(own_keys):
                    arrived(part, pk_s.at[NZ + n], pk_r.at[NZ + n])

            guard(q == 0, hold_own)

        arrived(vb.at[z, x, 1], ex_s.at[1], ex_r.at[1])
        for d in range(2):
            send(vb.at[z, x], xv_s.at[d], xv_r.at[d], xside[d])
        for d in range(2):
            vz_send(z, x, 1, 0, d)
        arrived(vb.at[z, xm], xv_s.at[0], xv_r.at[0])
        send(vb.at[z, xm, 0], xv_s.at[2], xv_r.at[2], xside[0])
        for d in range(2):
            vz_send(z, xm, 1, 1, d)
        arrived(vb.at[z, xp], xv_s.at[1], xv_r.at[1])
        send(vb.at[z, xp, 1], xv_s.at[3], xv_r.at[3], xside[1])
        for d in range(2):
            vz_send(z, xp, 1, 2, d)
        arrived(vb.at[z, xo, 0], xv_s.at[2], xv_r.at[2])
        arrived(vb.at[z, xo, 1], xv_s.at[3], xv_r.at[3])
        for d in range(2):
            vz_send(z, xo, 1, 3, d)
        for n, part in enumerate(own_values):
            send(part, pv_s.at[NZ + n], pv_r.at[NZ + n], partner)
        arrived(kb.at[z, x, pl.ds(DQK, DQK), :], ex_s.at[0], ex_r.at[0])
        loads[5].wait()

        def south_wait(s):
            if isinstance(s, int):
                return
            guard(s == 4, lambda: k_wait(0))
            guard(s >= 4, lambda: k_wait(s - 3))
            guard(s == 6, lambda: k_wait(s - 2))

        def round_of(s, forward):
            for col in range(4):
                for d in range(2):
                    zz = pull(s, d)
                    vz_wait(zz, cols[col], s, col, d)
                    if forward or col % 2 == d:
                        vz_send(zz, cols[col], s + 1, col, d)
                if col == 0:
                    south_wait(s)
            for d in range(2):
                p_send(pull(s, d))

        def loop_round(s, carry):
            round_of(s, True)
            return carry

        lax.fori_loop(1, 7, loop_round, 0)
        round_of(7, False)
        far = (z + 8) % NZ
        vz_wait(far, cols[0], 8, 0, 0)
        vz_wait(far, cols[1], 8, 1, 1)
        vz_wait(far, cols[2], 8, 2, 0)
        vz_wait(far, cols[3], 8, 3, 1)
        p_send(far)
        k_wait(5)
        k_wait(6)
        k_wait(7)
        k_wait(8)
        loads[2].wait()
        loads[3].wait()
        loads[4].wait()
        columns = jnp.concatenate(
            [g_vm[h] for h in range(HEADS)] + [jnp.zeros((4, ROWS), F32)], 0
        )
        gate_out[...] = jax.nn.sigmoid(jnp.transpose(columns))

        for k in range(1, NZ):
            zz = (z + k) % NZ
            left(vb.at[zz], pv_s.at[zz], pv_r.at[zz])
        for n, part in enumerate(own_values):
            left(part, pv_s.at[NZ + n], pv_r.at[NZ + n])
        for s in range(1, 9):
            for col in range(4):
                for d in range(2):
                    if s < 8 or col % 2 == d:
                        left(vb.at[z, x], zv_s.at[d, s, col], zv_r.at[d, s, col])
        for d in range(2):
            left(vb.at[z, x], xv_s.at[d], xv_r.at[d])
            left(vb.at[z, x, 0], xv_s.at[2 + d], xv_r.at[2 + d])
        left(own_k, ex_s.at[0], ex_r.at[0])
        left(own_v, ex_s.at[1], ex_r.at[1])
        left(halo_src, halo_s.at[0], halo_r.at[0])
        left(own_v.at[pl.ds(0, 16), :], halo_s.at[1], halo_r.at[1])


def mix_body(
    q_vm, kb, vb, gate_ref, picks_ref, out_ref, s_sc, p_sc, ks, vext, even_sc, odd_sc, bias_sc, comp_sc
):
    i = lax.axis_index("ctx")

    lane128 = lax.broadcasted_iota(jnp.int32, (256, 128), 1)
    wide_lane = lax.broadcasted_iota(jnp.int32, (ROWS, 128), 1)
    row_of = i * ROWS + lax.broadcasted_iota(jnp.int32, (ROWS, 128), 0)
    for part in range(4):
        rows = slice(256 * part, 256 * part + 256)

        def table(start):
            return jnp.concatenate(
                [
                    kb[4 * part + n // NX, n % NX, pl.ds(start, 16), :] for n in range(16)
                ],
                0,
            )

        ck0, ck1 = table(2 * DQK), table(2 * DQK + 16)
        vext[rows, :128] = table(2 * DQK + 32)
        even_sc[rows, :128] = ck0
        even_sc[rows, 128:] = ck1
        r0 = pltpu.roll(ck0.astype(F32), 64, 1)
        r1 = pltpu.roll(ck1.astype(F32), 64, 1)
        odd_sc[rows, :128] = jnp.where(lane128 < 64, r1, r0).astype(BF16)
        odd_sc[rows, 128:] = jnp.where(lane128 < 64, r0, r1).astype(BF16)
        for n in range(2):
            zed = 4 * part + 2 * n + wide_lane // 64
            block = (((wide_lane // 16) % 4) * 32 + zed * 2) * 8 + wide_lane % 16
            start = 256 * part + 128 * n
            bias_sc[:, start:start + 128] = jnp.where(block * 16 + 31 <= row_of, 0.0, LOW).astype(F32)
    vext[:, 128:] = jnp.ones((1024, 128), BF16)
    for par, table in ((0, even_sc), (1, odd_sc)):
        rows = jnp.concatenate(
            [q_vm[:, 384 * p + 128 * par:384 * p + 128 * par + 256] for p in range(PAIRS)], 0
        )
        s_sc[...] = lax.dot_general(
            rows, table[...], (((1,), (1,)), ((), ())), preferred_element_type=F32
        )
        for p in range(2 * PAIRS):
            rs = slice(64 * p, 64 * p + 64)
            score = s_sc[rs, :] + bias_sc[64 * (p % 2):64 * (p % 2) + 64, :]
            top_score = jnp.maximum(jnp.max(score, axis=1, keepdims=True), FLOOR)
            p_sc[rs, :] = jnp.exp2((score - top_score) * COEF).astype(BF16)
        result = jnp.dot(p_sc[...], vext[...], preferred_element_type=F32)
        for p in range(PAIRS):
            h = 2 * p + par
            rs = slice(128 * p, 128 * p + 128)
            comp = result[rs, :128] / jnp.maximum(result[rs, 128:], 1.0)
            comp_sc[h] = gate_ref[:, 2 * h:2 * h + 1] * comp

    ks[0:64, :] = jnp.zeros((64, 1024), BF16)
    ks[256:320, :] = jnp.zeros((64, 1024), BF16)
    half_lane = lax.broadcasted_iota(jnp.int32, (DQK, 128), 1)
    small_lane = lax.broadcasted_iota(jnp.int32, (TILE, 128), 1)
    small_row = lax.broadcasted_iota(jnp.int32, (TILE, 128), 0)
    for t in range(2):
        biases = []
        for j in range(PICKS // 2):
            tiles, sides = [], []
            for e in range(2):
                pick = picks_ref[t, 2 * j + e]
                safe = jnp.where(pick < 0, 2 * i + t, pick)
                owner = safe // 2
                part = safe % 2
                ox, oz, oc = owner // 32, (owner // 2) % NZ, owner % 2
                tile = kb[oz, ox, pl.ds(pl.multiple_of(oc * DQK, 64), DQK), :].astype(F32)
                shift = part * 64 if e == 0 else (1 - part) * 64
                tiles.append(pltpu.roll(tile, shift, 1))
                start = pl.multiple_of(part * 64, 64)
                vext[128 * j + 64 * e:128 * j + 64 * e + 64, :128] = vb[oz, ox, oc, pl.ds(start, 64), :]
                sides.append(jnp.where(pick < 0, LOW, 0.0).astype(F32))
            ks[64:256, 128 * j:128 * j + 128] = jnp.where(half_lane < 64, tiles[0], tiles[1]).astype(BF16)
            bias = jnp.where(small_lane < 64, sides[0], sides[1])
            if j == 0:
                bias = jnp.where((small_lane < 64) & (small_lane > small_row), LOW, bias)
            biases.append(bias)
        for par in range(2):
            rows = jnp.concatenate(
                [
                    q_vm[64 * t:64 * t + 64, 384 * p + 128 * par:384 * p + 128 * par + 256]
                    for p in range(PAIRS)
                ],
                0,
            )
            table = ks[64 - 64 * par:320 - 64 * par, :]
            s_sc[:448, :] = jnp.dot(rows, table, preferred_element_type=F32)
            for p in range(PAIRS):
                pieces = [
                    s_sc[64 * p:64 * p + 64, 128 * j:128 * j + 128] + biases[j]
                    for j in range(PICKS // 2)
                ]
                score = jnp.concatenate(pieces, 1)
                top_score = jnp.max(score, axis=1, keepdims=True)
                p_sc[64 * p:64 * p + 64, :] = jnp.exp2((score - top_score) * COEF).astype(BF16)
            result = jnp.dot(p_sc[:448, :], vext[...], preferred_element_type=F32)
            for p in range(PAIRS):
                h = 2 * p + par
                rs = slice(64 * t, 64 * t + 64)
                sel = result[64 * p:64 * p + 64, :128] / result[64 * p:64 * p + 64, 128:]
                mixed = comp_sc[h, rs] + gate_ref[rs, 2 * h + 1:2 * h + 2] * sel
                out_ref[rs, h * DV:(h + 1) * DV] = mixed.astype(BF16)


def local(queries, keys, values, key_weights, value_weights, picks, gates):
    vmem = pl.BlockSpec(memory_space=pltpu.VMEM)
    hbm = pl.BlockSpec(memory_space=pltpu.HBM)
    dma = pltpu.SemaphoreType.DMA
    kb, vb, rows, gate = pl.pallas_call(
        gather_body,
        out_shape=[
            pltpu.VMEM((NZ, NX, KROWS, 128), BF16),
            pltpu.VMEM((NZ, NX, 2, ROWS, 128), BF16),
            pltpu.VMEM((ROWS, HEADS * DQK), BF16),
            pltpu.VMEM((ROWS, 32), F32),
        ],
        in_specs=[hbm] * 6,
        out_specs=[vmem] * 4,
        scratch_shapes=[
            pltpu.VMEM((32, DQK), F32),
            pltpu.VMEM((32, DV), F32),
            pltpu.VMEM((HEADS, 2, ROWS), F32),
            pltpu.VMEM((16, DQK), BF16),
            pltpu.VMEM((16, DQK), BF16),
            pltpu.VMEM((16, DV), BF16),
            dma((6,)),
            dma((2,)), dma((2,)),
            dma((2,)), dma((2,)),
            dma((2, 9, 3)), dma((2, 9, 3)),
            dma((2, 9, 4)), dma((2, 9, 4)),
            dma((4,)), dma((4,)),
            dma((NZ, 3, 2)), dma((NZ, 3, 2)),
            dma((NZ + 4,)), dma((NZ + 4,)),
            dma((NZ + 3,)), dma((NZ + 3,)),
        ],
        compiler_params=pltpu.CompilerParams(
            collective_id=0, has_side_effects=True, vmem_limit_bytes=50 * 1024 * 1024
        ),
        name="gather_rows",
    )(queries, keys.T, values, key_weights, value_weights, jnp.transpose(gates, (2, 0, 1)))
    return pl.pallas_call(
        mix_body,
        out_shape=jax.ShapeDtypeStruct((ROWS, HEADS * DV), BF16),
        in_specs=[vmem] * 4 + [pl.BlockSpec(memory_space=pltpu.SMEM)],
        out_specs=vmem,
        scratch_shapes=[
            pltpu.VMEM((PAIRS * ROWS, 1024), F32),
            pltpu.VMEM((PAIRS * ROWS, 1024), BF16),
            pltpu.VMEM((320, 1024), BF16),
            pltpu.VMEM((1024, 256), BF16),
            pltpu.VMEM((1024, 256), BF16),
            pltpu.VMEM((1024, 256), BF16),
            pltpu.VMEM((ROWS, 1024), F32),
            pltpu.VMEM((HEADS, ROWS, 128), F32),
        ],
        compiler_params=pltpu.CompilerParams(vmem_limit_bytes=32 * 1024 * 1024),
        name="attend_mix",
    )(rows, kb, vb, gate, picks)


def solution(mesh):
    in_specs = (
        P("ctx", "kv"), P("ctx", "kv"), P("ctx", "kv"), P(None, "kv"), P(None, "kv"),
        P("ctx", None), P(None, "ctx", "kv"),
    )
    return jax.shard_map(
        local, mesh=mesh, in_specs=in_specs, out_specs=P("ctx", "kv"), check_vma=False
    )
```

```python
import jax
import jax.numpy as jnp
from jax import lax
from jax.experimental import pallas as pl
from jax.experimental.pallas import tpu as pltpu
from jax.sharding import PartitionSpec as P

NX = 4
NZ = 16
HEADS = 14
PAIRS = HEADS // 2
DQK = 192
DV = 128
ROWS = 128
TILE = 64
PICKS = 16
CROWS = 48
KROWS = 2 * DQK + CROWS
LOW = -1e30
FLOOR = -1e29
COEF = DQK ** (-0.5) * 1.4426950408889634
F32 = jnp.float32
BF16 = jnp.bfloat16
MESH = pl.DeviceIdType.MESH


def guard(cond, step):
    if isinstance(cond, bool):
        if cond:
            step()
    else:
        pl.when(cond)(step)


def gather_body(
    q_any, kt_any, v_any, kw_any, vw_any, g_any, picks_any,
    kb, vb, q_vm, gate_out, picks_out,
    kw, vw, g_vm, halo_src, halo_k, halo_v,
    in_s, halo_s, halo_r, ex_s, ex_r, zk_s, zk_r, zv_s, zv_r, xv_s, xv_r, xk_s, xk_r,
    pk_s, pk_r, pv_s, pv_r,
):
    i = lax.axis_index("ctx")
    x = i // 32
    z = (i // 2) % NZ
    c = i % 2

    def at(xx, zz, cc):
        return (xx % NX) * 32 + (zz % NZ) * 2 + cc

    zside = (at(x, z + 1, c), at(x, z + NZ - 1, c))
    xside = (at(x + 1, z, c), at(x + NX - 1, z, c))
    partner = at(x, z, 1 - c)
    before = (i + 127) % 128
    after = (i + 1) % 128
    xm, xp, xo = (x + 3) % NX, (x + 1) % NX, (x + 2) % NX
    cols = (x, xm, xp, xo)

    def remote(src, dst, ss, rs, target):
        return pltpu.make_async_remote_copy(
            src_ref=src, dst_ref=dst, send_sem=ss, recv_sem=rs,
            device_id={"ctx": target}, device_id_type=MESH,
        )

    def send(ref, ss, rs, target, dst=None):
        remote(ref, ref if dst is None else dst, ss, rs, target).start()

    def arrived(ref, ss, rs):
        remote(ref, ref, ss, rs, partner).wait_recv()

    def left(ref, ss, rs):
        remote(ref, ref, ss, rs, partner).wait_send()

    barrier = pltpu.get_barrier_semaphore()
    across = at(x + 2, z, c)
    for peer in (*zside, *xside, across, partner, before, after):
        pl.semaphore_signal(barrier, inc=1, device_id={"ctx": peer}, device_id_type=MESH)
    own_k = kb.at[z, x, pl.ds(pl.multiple_of(c * DQK, 64), DQK), :]
    own_v = vb.at[z, x, c]
    loads = [
        pltpu.make_async_copy(src, dst, in_s.at[n])
        for n, (src, dst) in enumerate([
            (kt_any, own_k), (v_any, own_v), (kw_any, kw), (vw_any, vw), (g_any, g_vm),
            (q_any, q_vm), (picks_any, picks_out),
        ])
    ]
    for load in loads:
        load.start()
    loads[0].wait()
    loads[1].wait()
    pl.semaphore_wait(barrier, 8)

    send(own_k, ex_s.at[0], ex_r.at[0], partner)
    send(own_v, ex_s.at[1], ex_r.at[1], partner)
    first_rows = own_v.at[pl.ds(0, 16), :]

    def natural_of(ref):
        return jnp.concatenate(
            [
                jnp.transpose(ref[pl.ds(0, 128), :].astype(F32)),
                jnp.transpose(ref[pl.ds(128, 64), :].astype(F32)),
            ],
            1,
        )

    def make_gate():
        loads[4].wait()
        stacked = jnp.concatenate(
            [g_vm[h] for h in range(HEADS)] + [jnp.zeros((4, ROWS), F32)], 0
        )
        gate_out[...] = jax.nn.sigmoid(jnp.transpose(stacked))

    own_keys = [kb.at[z, col] for col in cols[1:]] + [kb.at[z, x, pl.ds(2 * DQK, CROWS), :]]
    own_values = [vb.at[z, col] for col in cols[1:]]

    def pull(step, d):
        return (z + NZ - step) % NZ if d == 0 else (z + step) % NZ

    @pl.when(c == 1)
    def _():
        spans = (pl.ds(0, DQK), pl.ds(DQK, DQK), pl.ds(2 * DQK, CROWS))
        wide = (pl.ds(0, 2 * DQK), pl.ds(2 * DQK, CROWS))
        late = (0, 1, 1)

        def kz_send(zz, step, piece, d):
            part = kb.at[zz, x, spans[piece], :]
            send(part, zk_s.at[d, step, piece], zk_r.at[d, step, piece], zside[d])

        def kz_wait(zz, step, piece, d):
            part = kb.at[zz, x, spans[piece], :]
            arrived(part, zk_s.at[d, step, piece], zk_r.at[d, step, piece])

        def kx_send(zz, w):
            for d in range(2):
                send(kb.at[zz, x, wide[w], :], xk_s.at[zz, d, w], xk_r.at[zz, d, w], xside[d])

        def both(q, run):
            if isinstance(q, int):
                guard(q >= 0, lambda: run(pull(q, 0)))
                guard(0 < q < 8, lambda: run(pull(q, 1)))
            else:
                guard(q >= 0, lambda: run(pull(q, 0)))
                guard(q > 0, lambda: run(pull(q, 1)))

        def x_step(q, w):
            def move(zz):
                for d, col in ((0, xm), (1, xp)):
                    arrived(kb.at[zz, col, wide[w], :], xk_s.at[zz, d, w], xk_r.at[zz, d, w])
                sign = 1 - 2 * (zz % 2)
                origin = (x + NX - sign) % NX
                send(
                    kb.at[zz, origin, wide[w], :], xk_s.at[zz, 2, w], xk_r.at[zz, 2, w],
                    at(x + NX + sign, z, c),
                )

            both(q, move)

        def p_step(q):
            def landed(zz):
                for w in range(2):
                    arrived(kb.at[zz, xo, wide[w], :], xk_s.at[zz, 2, w], xk_r.at[zz, 2, w])

            def move(zz):
                landed(zz)
                send(kb.at[zz], pk_s.at[zz], pk_r.at[zz], partner)

            def move_own():
                landed(z)
                for n, part in enumerate(own_keys):
                    send(part, pk_s.at[NZ + n], pk_r.at[NZ + n], partner)

            if isinstance(q, int):
                guard(q > 0, lambda: move(pull(q, 0)))
                guard(0 < q < 8, lambda: move(pull(q, 1)))
            else:
                guard(q > 0, lambda: (move(pull(q, 0)), move(pull(q, 1)))[0])
            guard(q == 0, move_own)

        for d in range(2):
            kz_send(z, 1, 1, d)
        mine = natural_of(own_k)
        arrived(kb.at[z, x, spans[0], :], ex_s.at[0], ex_r.at[0])
        for d in range(2):
            kz_send(z, 1, 0, d)
        kx_send(z, 0)
        arrived(vb.at[z, x, 0], ex_s.at[1], ex_r.at[1])
        loads[2].wait()
        loads[3].wait()
        natural = jnp.concatenate([natural_of(kb.at[z, x, spans[0], :]), mine], 0)
        chip_v = jnp.concatenate([vb[z, x, 0], vb[z, x, 1]], 0).astype(F32)
        arrived(halo_k, halo_s.at[0], halo_r.at[0])
        arrived(halo_v, halo_s.at[1], halo_r.at[1])
        inside = (i != 127).astype(F32)

        def compress(rows, extra, weights):
            joined = jnp.concatenate([rows, extra.astype(F32) * inside], 0)
            parts = [
                jnp.sum(joined[16 * b:16 * b + 32] * weights, axis=0, keepdims=True)
                for b in range(16)
            ]
            return jnp.concatenate(parts, 0)

        ck = compress(natural, halo_k[...], kw[...])
        cv = compress(chip_v, halo_v[...], vw[...])
        own = kb.at[z, x]
        own[pl.ds(2 * DQK, 16), :] = ck[:, :128].astype(BF16)
        own[pl.ds(2 * DQK + 16, 16), :] = jnp.concatenate(
            [ck[:, 128:], jnp.zeros((16, 64), F32)], 1
        ).astype(BF16)
        own[pl.ds(2 * DQK + 32, 16), :] = cv.astype(BF16)
        for d in range(2):
            kz_send(z, 1, 2, d)
        kx_send(z, 1)
        left(own_k, ex_s.at[0], ex_r.at[0])
        left(own_v, ex_s.at[1], ex_r.at[1])

        def kz_left(step, pieces=(0, 1, 2)):
            for piece in pieces:
                for d in range(2):
                    if not isinstance(step, int) or step < 8 or late[piece] == d:
                        part = kb.at[z, x, spans[piece], :]
                        left(part, zk_s.at[d, step, piece], zk_r.at[d, step, piece])

        def kx_left(q, w):
            def run(zz):
                for d in range(3):
                    left(kb.at[zz, x, wide[w], :], xk_s.at[zz, d, w], xk_r.at[zz, d, w])

            both(q, run)

        def pk_left(q):
            def run(zz):
                left(kb.at[zz], pk_s.at[zz], pk_r.at[zz])

            def run_own():
                for n, part in enumerate(own_keys):
                    left(part, pk_s.at[NZ + n], pk_r.at[NZ + n])

            if isinstance(q, int):
                guard(q > 0, lambda: run(pull(q, 0)))
                guard(0 < q < 8, lambda: run(pull(q, 1)))
            else:
                guard(q > 0, lambda: (run(pull(q, 0)), run(pull(q, 1)))[0])
            guard(q == 0, run_own)

        def z_step(s, piece, forward):
            for d in range(2):
                zz = pull(s, d)
                kz_wait(zz, s, piece, d)
                if forward or late[piece] == d:
                    kz_send(zz, s + 1, piece, d)
                if piece != 1:
                    kx_send(zz, piece // 2)

        def round_of(s, forward):
            z_step(s, 1, forward)
            z_step(s, 0, forward)
            z_step(s, 2, forward)
            x_step(s - 1, 0)
            x_step(s - 2, 1)
            p_step(s - 3)
            guard(s >= 2, lambda: kz_left(s - 1))
            kx_left(s - 2, 0)
            kx_left(s - 3, 1)
            pk_left(s - 4)

        def loop_round(s, carry):
            round_of(s, True)
            return carry

        lax.fori_loop(1, 7, loop_round, 0)
        round_of(7, False)
        far = (z + 8) % NZ
        kz_wait(far, 8, 1, 1)
        kz_wait(far, 8, 0, 0)
        kx_send(far, 0)
        kz_wait(far, 8, 2, 1)
        kx_send(far, 1)
        make_gate()
        loads[5].wait()
        loads[6].wait()
        for s in range(8, 9 + 3):
            if s - 1 <= 8:
                x_step(s - 1, 0)
            if s - 2 <= 8:
                x_step(s - 2, 1)
            if s - 3 <= 8:
                p_step(s - 3)
        kz_left(7)
        kz_left(8)
        for q in range(max(0, 6), 9):
            kx_left(q, 0)
        for q in range(max(0, 5), 9):
            kx_left(q, 1)
        for q in range(max(0, 4), 9):
            pk_left(q)
        for k in range(1, NZ):
            zz = (z + k) % NZ
            arrived(vb.at[zz], pv_s.at[zz], pv_r.at[zz])
        for n, part in enumerate(own_values):
            arrived(part, pv_s.at[NZ + n], pv_r.at[NZ + n])

    @pl.when(c == 0)
    def _():
        def vz_send(zz, xx, step, col, d):
            send(vb.at[zz, xx], zv_s.at[d, step, col], zv_r.at[d, step, col], zside[d])

        def vz_wait(zz, xx, step, col, d):
            arrived(vb.at[zz, xx], zv_s.at[d, step, col], zv_r.at[d, step, col])

        def p_send(zz):
            send(vb.at[zz], pv_s.at[zz], pv_r.at[zz], partner)

        def k_wait(q):
            for d in range(2):
                zz = pull(q, d)

                def hold(zz=zz):
                    arrived(kb.at[zz], pk_s.at[zz], pk_r.at[zz])

                guard(q > 0 if d == 0 or not isinstance(q, int) else 0 < q < 8, hold)

            def hold_own():
                for n, part in enumerate(own_keys):
                    arrived(part, pk_s.at[NZ + n], pk_r.at[NZ + n])

            guard(q == 0, hold_own)

        send(first_rows, halo_s.at[1], halo_r.at[1], before, halo_v)
        halo_src[...] = natural_of(own_k)[:16].astype(BF16)
        arrived(vb.at[z, x, 1], ex_s.at[1], ex_r.at[1])
        for d in range(2):
            send(vb.at[z, x], xv_s.at[d], xv_r.at[d], xside[d])
        send(vb.at[z, x], xv_s.at[2], xv_r.at[2], across)
        for d in range(2):
            vz_send(z, x, 1, 0, d)
        send(halo_src, halo_s.at[0], halo_r.at[0], before, halo_k)
        arrived(vb.at[z, xm], xv_s.at[0], xv_r.at[0])
        for d in range(2):
            vz_send(z, xm, 1, 1, d)
        arrived(vb.at[z, xp], xv_s.at[1], xv_r.at[1])
        for d in range(2):
            vz_send(z, xp, 1, 2, d)
        arrived(vb.at[z, xo], xv_s.at[2], xv_r.at[2])
        for d in range(2):
            vz_send(z, xo, 1, 3, d)
        for n, part in enumerate(own_values):
            send(part, pv_s.at[NZ + n], pv_r.at[NZ + n], partner)
        arrived(kb.at[z, x, pl.ds(DQK, DQK), :], ex_s.at[0], ex_r.at[0])
        for d in range(3):
            left(vb.at[z, x], xv_s.at[d], xv_r.at[d])
        left(own_k, ex_s.at[0], ex_r.at[0])
        left(own_v, ex_s.at[1], ex_r.at[1])
        left(halo_src, halo_s.at[0], halo_r.at[0])
        left(first_rows, halo_s.at[1], halo_r.at[1])

        def vz_left(step):
            for col in range(4):
                for d in range(2):
                    if not isinstance(step, int) or step < 8 or col % 2 == d:
                        left(vb.at[z, x], zv_s.at[d, step, col], zv_r.at[d, step, col])

        def pv_left(step):
            zz = pull(step, 0)
            left(vb.at[zz], pv_s.at[zz], pv_r.at[zz])
            if not isinstance(step, int) or step != 8:
                zz = pull(step, 1)
                left(vb.at[zz], pv_s.at[zz], pv_r.at[zz])

        def round_of(s, forward):
            for col in range(4):
                for d in range(2):
                    zz = pull(s, d)
                    vz_wait(zz, cols[col], s, col, d)
                    if forward or col % 2 == d:
                        vz_send(zz, cols[col], s + 1, col, d)
            for d in range(2):
                p_send(pull(s, d))
            guard(s >= 2, lambda: vz_left(s - 1))
            guard(s >= 3, lambda: pv_left(s - 2))

        def loop_round(s, carry):
            round_of(s, True)
            return carry

        lax.fori_loop(1, 7, loop_round, 0)
        round_of(7, False)
        far = (z + 8) % NZ
        make_gate()
        for load in (loads[2], loads[3], loads[5], loads[6]):
            load.wait()
        vz_wait(far, cols[0], 8, 0, 0)
        vz_wait(far, cols[1], 8, 1, 1)
        vz_wait(far, cols[2], 8, 2, 0)
        vz_wait(far, cols[3], 8, 3, 1)
        p_send(far)
        for n, part in enumerate(own_values):
            left(part, pv_s.at[NZ + n], pv_r.at[NZ + n])
        for step in range(6, 9):
            pv_left(step)
        vz_left(7)
        vz_left(8)
        for q in range(9):
            k_wait(q)


def mix_body(
    q_vm, kb, vb, gate_ref, picks_ref, out_ref, s_sc, p_sc, ks, vext, even_sc, odd_sc, bias_sc, comp_sc
):
    i = lax.axis_index("ctx")
    for n in range(3):
        vext[n, :, 128:] = jnp.ones((1024, 128), BF16)
    for n in range(2):
        ks[n, 0:64, :] = jnp.zeros((64, 1024), BF16)
        ks[n, 256:320, :] = jnp.zeros((64, 1024), BF16)

    lane128 = lax.broadcasted_iota(jnp.int32, (256, 128), 1)
    wide_lane = lax.broadcasted_iota(jnp.int32, (ROWS, 128), 1)
    row_of = i * ROWS + lax.broadcasted_iota(jnp.int32, (ROWS, 128), 0)
    for part in range(4):
        rows = slice(256 * part, 256 * part + 256)

        def table(start):
            return jnp.concatenate(
                [
                    kb[4 * part + n // NX, n % NX, pl.ds(start, 16), :] for n in range(16)
                ],
                0,
            )

        ck0, ck1 = table(2 * DQK), table(2 * DQK + 16)
        vext[2, rows, :128] = table(2 * DQK + 32)
        even_sc[rows, :128] = ck0
        even_sc[rows, 128:] = ck1
        r0 = pltpu.roll(ck0.astype(F32), 64, 1)
        r1 = pltpu.roll(ck1.astype(F32), 64, 1)
        odd_sc[rows, :128] = jnp.where(lane128 < 64, r1, r0).astype(BF16)
        odd_sc[rows, 128:] = jnp.where(lane128 < 64, r0, r1).astype(BF16)
        for n in range(2):
            zed = 4 * part + 2 * n + wide_lane // 64
            block = (((wide_lane // 16) % 4) * 32 + zed * 2) * 8 + wide_lane % 16
            start = 256 * part + 128 * n
            bias_sc[:, start:start + 128] = jnp.where(block * 16 + 31 <= row_of, 0.0, LOW).astype(F32)

    half_lane = lax.broadcasted_iota(jnp.int32, (DQK, 128), 1)
    small_lane = lax.broadcasted_iota(jnp.int32, (TILE, 128), 1)
    small_row = lax.broadcasted_iota(jnp.int32, (TILE, 128), 0)
    biases = {0: [], 1: []}

    def pick_tables(t):
        for j in range(PICKS // 2):
            tiles, sides = [], []
            for e in range(2):
                pick = picks_ref[t, 2 * j + e]
                safe = jnp.where(pick < 0, 2 * i + t, pick)
                owner = safe // 2
                part = safe % 2
                ox, oz, oc = owner // 32, (owner // 2) % NZ, owner % 2
                tile = kb[oz, ox, pl.ds(pl.multiple_of(oc * DQK, 64), DQK), :].astype(F32)
                shift = part * 64 if e == 0 else (1 - part) * 64
                tiles.append(pltpu.roll(tile, shift, 1))
                start = pl.multiple_of(part * 64, 64)
                at = 128 * j + 64 * e
                vext[t, at:at + 64, :128] = vb[oz, ox, oc, pl.ds(start, 64), :]
                sides.append(jnp.where(pick < 0, LOW, 0.0).astype(F32))
            ks[t, 64:256, 128 * j:128 * j + 128] = jnp.where(
                half_lane < 64, tiles[0], tiles[1]
            ).astype(BF16)
            bias = jnp.where(small_lane < 64, sides[0], sides[1])
            if j == 0:
                bias = jnp.where((small_lane < 64) & (small_lane > small_row), LOW, bias)
            biases[t].append(bias)

    def queries_of(start, count, par):
        return jnp.concatenate(
            [
                q_vm[start:start + count, 384 * p + 128 * par:384 * p + 128 * par + 256]
                for p in range(PAIRS)
            ],
            0,
        )

    def scores(stage, buf):
        kind, par = stage
        if kind == 2:
            table = (even_sc, odd_sc)[par]
            s_sc[buf] = lax.dot_general(
                queries_of(0, ROWS, par), table[...], (((1,), (1,)), ((), ())),
                preferred_element_type=F32,
            )
        else:
            table = ks[kind, 64 - 64 * par:320 - 64 * par, :]
            s_sc[buf, :448, :] = jnp.dot(
                queries_of(64 * kind, 64, par), table, preferred_element_type=F32
            )

    def finish(stage, buf):
        kind, par = stage
        count = 2 * PAIRS if kind == 2 else PAIRS
        for p in range(count):
            rs = slice(64 * p, 64 * p + 64)
            if kind == 2:
                score = s_sc[buf, rs, :] + bias_sc[64 * (p % 2):64 * (p % 2) + 64, :]
            else:
                score = jnp.concatenate(
                    [
                        s_sc[buf, rs, 128 * j:128 * j + 128] + biases[kind][j]
                        for j in range(PICKS // 2)
                    ],
                    1,
                )
            top_score = jnp.maximum(jnp.max(score, axis=1, keepdims=True), FLOOR)
            p_sc[buf, rs, :] = jnp.exp2((score - top_score) * COEF).astype(BF16)
        result = jnp.dot(p_sc[buf, :64 * count, :], vext[kind], preferred_element_type=F32)
        for p in range(PAIRS):
            h = 2 * p + par
            if kind == 2:
                rs = slice(128 * p, 128 * p + 128)
                comp = result[rs, :128] / jnp.maximum(result[rs, 128:], 1.0)
                comp_sc[h] = gate_ref[:, 2 * h:2 * h + 1] * comp
            else:
                rs = slice(64 * kind, 64 * kind + 64)
                sel = result[64 * p:64 * p + 64, :128] / result[64 * p:64 * p + 64, 128:]
                mixed = comp_sc[h, rs] + gate_ref[rs, 2 * h + 1:2 * h + 2] * sel
                out_ref[rs, h * DV:(h + 1) * DV] = mixed.astype(BF16)

    stages = [(2, 0), (2, 1), (0, 0), (0, 1), (1, 0), (1, 1)]
    for n, stage in enumerate(stages):
        if n == 0:
            scores(stage, 0)
            pick_tables(0)
        if n + 1 < len(stages):
            scores(stages[n + 1], (n + 1) % 2)
        if n == 1:
            pick_tables(1)
        finish(stage, n % 2)


def local(queries, keys, values, key_weights, value_weights, picks, gates):
    vmem = pl.BlockSpec(memory_space=pltpu.VMEM)
    hbm = pl.BlockSpec(memory_space=pltpu.HBM)
    dma = pltpu.SemaphoreType.DMA
    kb, vb, rows, gate, listed = pl.pallas_call(
        gather_body,
        out_shape=[
            pltpu.VMEM((NZ, NX, KROWS, 128), BF16),
            pltpu.VMEM((NZ, NX, 2, ROWS, 128), BF16),
            pltpu.VMEM((ROWS, HEADS * DQK), BF16),
            pltpu.VMEM((ROWS, 32), F32),
            pltpu.SMEM((2, PICKS), jnp.int32),
        ],
        in_specs=[hbm] * 7,
        out_specs=[vmem] * 4 + [pl.BlockSpec(memory_space=pltpu.SMEM)],
        scratch_shapes=[
            pltpu.VMEM((32, DQK), F32),
            pltpu.VMEM((32, DV), F32),
            pltpu.VMEM((HEADS, 2, ROWS), F32),
            pltpu.VMEM((16, DQK), BF16),
            pltpu.VMEM((16, DQK), BF16),
            pltpu.VMEM((16, DV), BF16),
            dma((7,)),
            dma((2,)), dma((2,)),
            dma((2,)), dma((2,)),
            dma((2, 9, 3)), dma((2, 9, 3)),
            dma((2, 9, 4)), dma((2, 9, 4)),
            dma((3,)), dma((3,)),
            dma((NZ, 3, 2)), dma((NZ, 3, 2)),
            dma((NZ + 4,)), dma((NZ + 4,)),
            dma((NZ + 3,)), dma((NZ + 3,)),
        ],
        compiler_params=pltpu.CompilerParams(
            collective_id=0, has_side_effects=True, vmem_limit_bytes=50 * 1024 * 1024
        ),
        name="gather_rows",
    )(queries, keys.T, values, key_weights, value_weights, jnp.transpose(gates, (2, 0, 1)), picks)
    return pl.pallas_call(
        mix_body,
        out_shape=jax.ShapeDtypeStruct((ROWS, HEADS * DV), BF16),
        in_specs=[vmem] * 4 + [pl.BlockSpec(memory_space=pltpu.SMEM)],
        out_specs=vmem,
        scratch_shapes=[
            pltpu.VMEM((2, PAIRS * ROWS, 1024), F32),
            pltpu.VMEM((2, PAIRS * ROWS, 1024), BF16),
            pltpu.VMEM((2, 320, 1024), BF16),
            pltpu.VMEM((3, 1024, 256), BF16),
            pltpu.VMEM((1024, 256), BF16),
            pltpu.VMEM((1024, 256), BF16),
            pltpu.VMEM((ROWS, 1024), F32),
            pltpu.VMEM((HEADS, ROWS, 128), F32),
        ],
        compiler_params=pltpu.CompilerParams(vmem_limit_bytes=32 * 1024 * 1024),
        name="attend_mix",
    )(rows, kb, vb, gate, listed)


def solution(mesh):
    in_specs = (
        P("ctx", "kv"), P("ctx", "kv"), P("ctx", "kv"), P(None, "kv"), P(None, "kv"),
        P("ctx", None), P(None, "ctx", "kv"),
    )
    return jax.shard_map(
        local, mesh=mesh, in_specs=in_specs, out_specs=P("ctx", "kv"), check_vma=False
    )
```

```python
import jax
import jax.numpy as jnp
from jax import lax
from jax.experimental import pallas as pl
from jax.experimental.pallas import tpu as pltpu
from jax.sharding import PartitionSpec as P

NX = 4
NZ = 16
HEADS = 14
PAIRS = HEADS // 2
DQK = 192
DV = 128
ROWS = 128
TILE = 64
PICKS = 16
CROWS = 48
KROWS = 2 * DQK + CROWS
LOW = -1e30
FLOOR = -1e29
COEF = DQK ** (-0.5) * 1.4426950408889634
F32 = jnp.float32
BF16 = jnp.bfloat16
MESH = pl.DeviceIdType.MESH


def guard(cond, step):
    if isinstance(cond, bool):
        if cond:
            step()
    else:
        pl.when(cond)(step)


def gather_body(
    q_any, kt_any, v_any, kw_any, vw_any, g_any, picks_any,
    kb, vb, q_vm, gate_out, picks_out,
    kw, vw, g_vm, halo_src, halo_k, halo_v,
    in_s, halo_s, halo_r, ex_s, ex_r, zk_s, zk_r, zv_s, zv_r, xv_s, xv_r, xk_s, xk_r,
    pk_s, pk_r, pv_s, pv_r,
):
    i = lax.axis_index("ctx")
    x = i // 32
    z = (i // 2) % NZ
    c = i % 2

    def at(xx, zz, cc):
        return (xx % NX) * 32 + (zz % NZ) * 2 + cc

    zside = (at(x, z + 1, c), at(x, z + NZ - 1, c))
    xside = (at(x + 1, z, c), at(x + NX - 1, z, c))
    partner = at(x, z, 1 - c)
    before = (i + 127) % 128
    after = (i + 1) % 128
    xm, xp, xo = (x + 3) % NX, (x + 1) % NX, (x + 2) % NX
    cols = (x, xm, xp, xo)

    def remote(src, dst, ss, rs, target):
        return pltpu.make_async_remote_copy(
            src_ref=src, dst_ref=dst, send_sem=ss, recv_sem=rs,
            device_id={"ctx": target}, device_id_type=MESH,
        )

    def send(ref, ss, rs, target, dst=None):
        remote(ref, ref if dst is None else dst, ss, rs, target).start()

    def arrived(ref, ss, rs):
        remote(ref, ref, ss, rs, partner).wait_recv()

    def left(ref, ss, rs):
        remote(ref, ref, ss, rs, partner).wait_send()

    barrier = pltpu.get_barrier_semaphore()
    across = at(x + 2, z, c)
    for peer in (*zside, *xside, across, partner, before, after):
        pl.semaphore_signal(barrier, inc=1, device_id={"ctx": peer}, device_id_type=MESH)
    own_k = kb.at[z, x, pl.ds(pl.multiple_of(c * DQK, 64), DQK), :]
    own_v = vb.at[z, x, c]
    loads = [
        pltpu.make_async_copy(src, dst, in_s.at[n])
        for n, (src, dst) in enumerate([
            (kt_any, own_k), (v_any, own_v), (kw_any, kw), (vw_any, vw), (g_any, g_vm),
            (q_any, q_vm), (picks_any, picks_out),
        ])
    ]
    for load in loads:
        load.start()
    loads[0].wait()
    loads[1].wait()
    pl.semaphore_wait(barrier, 8)

    send(own_k, ex_s.at[0], ex_r.at[0], partner)
    send(own_v, ex_s.at[1], ex_r.at[1], partner)
    first_rows = own_v.at[pl.ds(0, 16), :]

    def natural_of(ref):
        return jnp.concatenate(
            [
                jnp.transpose(ref[pl.ds(0, 128), :].astype(F32)),
                jnp.transpose(ref[pl.ds(128, 64), :].astype(F32)),
            ],
            1,
        )

    def make_gate():
        loads[4].wait()
        stacked = jnp.concatenate(
            [g_vm[h] for h in range(HEADS)] + [jnp.zeros((4, ROWS), F32)], 0
        )
        gate_out[...] = jax.nn.sigmoid(jnp.transpose(stacked))

    own_keys = [kb.at[z, col] for col in cols[1:]] + [kb.at[z, x, pl.ds(2 * DQK, CROWS), :]]
    own_values = [vb.at[z, col] for col in cols[1:]]
    last = (z + 8) % NZ
    last_keys = [kb.at[last, col] for col in cols]
    last_values = [vb.at[last, col] for col in cols]

    def pull(step, d):
        return (z + NZ - step) % NZ if d == 0 else (z + step) % NZ

    @pl.when(c == 1)
    def _():
        spans = (pl.ds(0, DQK), pl.ds(DQK, DQK), pl.ds(2 * DQK, CROWS))
        wide = (pl.ds(0, 2 * DQK), pl.ds(2 * DQK, CROWS))
        late = (0, 1, 1)

        def kz_send(zz, step, piece, d):
            part = kb.at[zz, x, spans[piece], :]
            send(part, zk_s.at[d, step, piece], zk_r.at[d, step, piece], zside[d])

        def kz_wait(zz, step, piece, d):
            part = kb.at[zz, x, spans[piece], :]
            arrived(part, zk_s.at[d, step, piece], zk_r.at[d, step, piece])

        def kx_send(zz, w):
            for d in range(2):
                send(kb.at[zz, x, wide[w], :], xk_s.at[zz, d, w], xk_r.at[zz, d, w], xside[d])

        def both(q, run):
            if isinstance(q, int):
                guard(q >= 0, lambda: run(pull(q, 0)))
                guard(0 < q < 8, lambda: run(pull(q, 1)))
            else:
                guard(q >= 0, lambda: run(pull(q, 0)))
                guard(q > 0, lambda: run(pull(q, 1)))

        def x_step(q, w):
            def move(zz):
                for d, col in ((0, xm), (1, xp)):
                    arrived(kb.at[zz, col, wide[w], :], xk_s.at[zz, d, w], xk_r.at[zz, d, w])
                sign = 1 - 2 * (zz % 2)
                origin = (x + NX - sign) % NX
                send(
                    kb.at[zz, origin, wide[w], :], xk_s.at[zz, 2, w], xk_r.at[zz, 2, w],
                    at(x + NX + sign, z, c),
                )

            both(q, move)

        def p_step(q):
            def landed(zz):
                for w in range(2):
                    arrived(kb.at[zz, xo, wide[w], :], xk_s.at[zz, 2, w], xk_r.at[zz, 2, w])

            def move(zz):
                landed(zz)
                send(kb.at[zz], pk_s.at[zz], pk_r.at[zz], partner)

            def move_own():
                landed(z)
                for n, part in enumerate(own_keys):
                    send(part, pk_s.at[NZ + n], pk_r.at[NZ + n], partner)

            if isinstance(q, int):
                guard(0 < q < 8, lambda: move(pull(q, 0)))
                guard(0 < q < 8, lambda: move(pull(q, 1)))
                if q == 8:
                    for n in range(3):
                        send(last_keys[n], pk_s.at[NZ + 4 + n], pk_r.at[NZ + 4 + n], partner)
                    landed(last)
                    send(last_keys[3], pk_s.at[NZ + 7], pk_r.at[NZ + 7], partner)
            else:
                guard(q > 0, lambda: (move(pull(q, 0)), move(pull(q, 1)))[0])
            guard(q == 0, move_own)

        for d in range(2):
            kz_send(z, 1, 1, d)
        mine = natural_of(own_k)
        arrived(kb.at[z, x, spans[0], :], ex_s.at[0], ex_r.at[0])
        for d in range(2):
            kz_send(z, 1, 0, d)
        kx_send(z, 0)
        arrived(vb.at[z, x, 0], ex_s.at[1], ex_r.at[1])
        loads[2].wait()
        loads[3].wait()
        natural = jnp.concatenate([natural_of(kb.at[z, x, spans[0], :]), mine], 0)
        chip_v = jnp.concatenate([vb[z, x, 0], vb[z, x, 1]], 0).astype(F32)
        arrived(halo_k, halo_s.at[0], halo_r.at[0])
        arrived(halo_v, halo_s.at[1], halo_r.at[1])
        inside = (i != 127).astype(F32)

        def compress(rows, extra, weights):
            joined = jnp.concatenate([rows, extra.astype(F32) * inside], 0)
            parts = [
                jnp.sum(joined[16 * b:16 * b + 32] * weights, axis=0, keepdims=True)
                for b in range(16)
            ]
            return jnp.concatenate(parts, 0)

        ck = compress(natural, halo_k[...], kw[...])
        cv = compress(chip_v, halo_v[...], vw[...])
        own = kb.at[z, x]
        own[pl.ds(2 * DQK, 16), :] = ck[:, :128].astype(BF16)
        own[pl.ds(2 * DQK + 16, 16), :] = jnp.concatenate(
            [ck[:, 128:], jnp.zeros((16, 64), F32)], 1
        ).astype(BF16)
        own[pl.ds(2 * DQK + 32, 16), :] = cv.astype(BF16)
        for d in range(2):
            kz_send(z, 1, 2, d)
        kx_send(z, 1)
        left(own_k, ex_s.at[0], ex_r.at[0])
        left(own_v, ex_s.at[1], ex_r.at[1])

        def kz_left(step, pieces=(0, 1, 2)):
            for piece in pieces:
                for d in range(2):
                    if not isinstance(step, int) or step < 8 or late[piece] == d:
                        part = kb.at[z, x, spans[piece], :]
                        left(part, zk_s.at[d, step, piece], zk_r.at[d, step, piece])

        def kx_left(q, w):
            def run(zz):
                for d in range(3):
                    left(kb.at[zz, x, wide[w], :], xk_s.at[zz, d, w], xk_r.at[zz, d, w])

            both(q, run)

        def pk_left(q):
            def run(zz):
                left(kb.at[zz], pk_s.at[zz], pk_r.at[zz])

            def run_own():
                for n, part in enumerate(own_keys):
                    left(part, pk_s.at[NZ + n], pk_r.at[NZ + n])

            if isinstance(q, int):
                guard(0 < q < 8, lambda: run(pull(q, 0)))
                guard(0 < q < 8, lambda: run(pull(q, 1)))
                if q == 8:
                    for n, part in enumerate(last_keys):
                        left(part, pk_s.at[NZ + 4 + n], pk_r.at[NZ + 4 + n])
            else:
                guard(q > 0, lambda: (run(pull(q, 0)), run(pull(q, 1)))[0])
            guard(q == 0, run_own)

        def z_step(s, piece, forward):
            for d in range(2):
                zz = pull(s, d)
                kz_wait(zz, s, piece, d)
                if forward or late[piece] == d:
                    kz_send(zz, s + 1, piece, d)
                if piece != 1:
                    kx_send(zz, piece // 2)

        def round_of(s, forward):
            z_step(s, 1, forward)
            z_step(s, 0, forward)
            z_step(s, 2, forward)
            x_step(s - 1, 0)
            x_step(s - 2, 1)
            p_step(s - 3)
            guard(s >= 2, lambda: kz_left(s - 1))
            kx_left(s - 2, 0)
            kx_left(s - 3, 1)
            pk_left(s - 4)

        def loop_round(s, carry):
            round_of(s, True)
            return carry

        lax.fori_loop(1, 7, loop_round, 0)
        round_of(7, False)
        far = (z + 8) % NZ
        kz_wait(far, 8, 1, 1)
        kz_wait(far, 8, 0, 0)
        kx_send(far, 0)
        kz_wait(far, 8, 2, 1)
        kx_send(far, 1)
        make_gate()
        loads[5].wait()
        loads[6].wait()
        for s in range(8, 9 + 3):
            if s - 1 <= 8:
                x_step(s - 1, 0)
            if s - 2 <= 8:
                x_step(s - 2, 1)
            if s - 3 <= 8:
                p_step(s - 3)
        kz_left(7)
        kz_left(8)
        for q in range(max(0, 6), 9):
            kx_left(q, 0)
        for q in range(max(0, 5), 9):
            kx_left(q, 1)
        for q in range(max(0, 4), 9):
            pk_left(q)
        for k in range(1, NZ):
            if k != 8:
                zz = (z + k) % NZ
                arrived(vb.at[zz], pv_s.at[zz], pv_r.at[zz])
        for n, part in enumerate(last_values):
            arrived(part, pv_s.at[NZ + 3 + n], pv_r.at[NZ + 3 + n])
        for n, part in enumerate(own_values):
            arrived(part, pv_s.at[NZ + n], pv_r.at[NZ + n])

    @pl.when(c == 0)
    def _():
        def vz_send(zz, xx, step, col, d):
            send(vb.at[zz, xx], zv_s.at[d, step, col], zv_r.at[d, step, col], zside[d])

        def vz_wait(zz, xx, step, col, d):
            arrived(vb.at[zz, xx], zv_s.at[d, step, col], zv_r.at[d, step, col])

        def p_send(zz):
            send(vb.at[zz], pv_s.at[zz], pv_r.at[zz], partner)

        def k_wait(q):
            if 0 < q < 8:
                for d in range(2):
                    zz = pull(q, d)
                    arrived(kb.at[zz], pk_s.at[zz], pk_r.at[zz])
            if q == 8:
                for n, part in enumerate(last_keys):
                    arrived(part, pk_s.at[NZ + 4 + n], pk_r.at[NZ + 4 + n])

            def hold_own():
                for n, part in enumerate(own_keys):
                    arrived(part, pk_s.at[NZ + n], pk_r.at[NZ + n])

            guard(q == 0, hold_own)

        send(first_rows, halo_s.at[1], halo_r.at[1], before, halo_v)
        halo_src[...] = natural_of(own_k)[:16].astype(BF16)
        arrived(vb.at[z, x, 1], ex_s.at[1], ex_r.at[1])
        for d in range(2):
            send(vb.at[z, x], xv_s.at[d], xv_r.at[d], xside[d])
        send(vb.at[z, x], xv_s.at[2], xv_r.at[2], across)
        for d in range(2):
            vz_send(z, x, 1, 0, d)
        send(halo_src, halo_s.at[0], halo_r.at[0], before, halo_k)
        arrived(vb.at[z, xm], xv_s.at[0], xv_r.at[0])
        for d in range(2):
            vz_send(z, xm, 1, 1, d)
        arrived(vb.at[z, xp], xv_s.at[1], xv_r.at[1])
        for d in range(2):
            vz_send(z, xp, 1, 2, d)
        arrived(vb.at[z, xo], xv_s.at[2], xv_r.at[2])
        for d in range(2):
            vz_send(z, xo, 1, 3, d)
        for n, part in enumerate(own_values):
            send(part, pv_s.at[NZ + n], pv_r.at[NZ + n], partner)
        arrived(kb.at[z, x, pl.ds(DQK, DQK), :], ex_s.at[0], ex_r.at[0])
        for d in range(3):
            left(vb.at[z, x], xv_s.at[d], xv_r.at[d])
        left(own_k, ex_s.at[0], ex_r.at[0])
        left(own_v, ex_s.at[1], ex_r.at[1])
        left(halo_src, halo_s.at[0], halo_r.at[0])
        left(first_rows, halo_s.at[1], halo_r.at[1])

        def vz_left(step):
            for col in range(4):
                for d in range(2):
                    if not isinstance(step, int) or step < 8 or col % 2 == d:
                        left(vb.at[z, x], zv_s.at[d, step, col], zv_r.at[d, step, col])

        def pv_left(step):
            zz = pull(step, 0)
            left(vb.at[zz], pv_s.at[zz], pv_r.at[zz])
            if not isinstance(step, int) or step != 8:
                zz = pull(step, 1)
                left(vb.at[zz], pv_s.at[zz], pv_r.at[zz])

        def round_of(s, forward):
            for col in range(4):
                for d in range(2):
                    zz = pull(s, d)
                    vz_wait(zz, cols[col], s, col, d)
                    if forward or col % 2 == d:
                        vz_send(zz, cols[col], s + 1, col, d)
            for d in range(2):
                p_send(pull(s, d))
            guard(s >= 2, lambda: vz_left(s - 1))
            guard(s >= 3, lambda: pv_left(s - 2))

        def loop_round(s, carry):
            round_of(s, True)
            return carry

        lax.fori_loop(1, 7, loop_round, 0)
        round_of(7, False)
        far = (z + 8) % NZ
        make_gate()
        for load in (loads[2], loads[3], loads[5], loads[6]):
            load.wait()
        for n, part in enumerate(last_values):
            vz_wait(far, cols[n], 8, n, n % 2)
            send(part, pv_s.at[NZ + 3 + n], pv_r.at[NZ + 3 + n], partner)
        for n, part in enumerate(own_values):
            left(part, pv_s.at[NZ + n], pv_r.at[NZ + n])
        for step in range(6, 8):
            pv_left(step)
        for n, part in enumerate(last_values):
            left(part, pv_s.at[NZ + 3 + n], pv_r.at[NZ + 3 + n])
        vz_left(7)
        vz_left(8)
        for q in range(9):
            k_wait(q)


def mix_body(
    q_vm, kb, vb, gate_ref, picks_ref, out_ref, s_sc, p_sc, ks, vext, even_sc, odd_sc, bias_sc, comp_sc
):
    i = lax.axis_index("ctx")
    for n in range(3):
        vext[n, :, 128:] = jnp.ones((1024, 128), BF16)
    for n in range(2):
        ks[n, 0:64, :] = jnp.zeros((64, 1024), BF16)
        ks[n, 256:320, :] = jnp.zeros((64, 1024), BF16)

    lane128 = lax.broadcasted_iota(jnp.int32, (256, 128), 1)
    wide_lane = lax.broadcasted_iota(jnp.int32, (ROWS, 128), 1)
    row_of = i * ROWS + lax.broadcasted_iota(jnp.int32, (ROWS, 128), 0)
    for part in range(4):
        rows = slice(256 * part, 256 * part + 256)

        def table(start):
            return jnp.concatenate(
                [
                    kb[4 * part + n // NX, n % NX, pl.ds(start, 16), :] for n in range(16)
                ],
                0,
            )

        ck0, ck1 = table(2 * DQK), table(2 * DQK + 16)
        vext[2, rows, :128] = table(2 * DQK + 32)
        even_sc[rows, :128] = ck0
        even_sc[rows, 128:] = ck1
        r0 = pltpu.roll(ck0.astype(F32), 64, 1)
        r1 = pltpu.roll(ck1.astype(F32), 64, 1)
        odd_sc[rows, :128] = jnp.where(lane128 < 64, r1, r0).astype(BF16)
        odd_sc[rows, 128:] = jnp.where(lane128 < 64, r0, r1).astype(BF16)
        for n in range(2):
            zed = 4 * part + 2 * n + wide_lane // 64
            block = (((wide_lane // 16) % 4) * 32 + zed * 2) * 8 + wide_lane % 16
            start = 256 * part + 128 * n
            bias_sc[:, start:start + 128] = jnp.where(block * 16 + 31 <= row_of, 0.0, LOW).astype(F32)

    half_lane = lax.broadcasted_iota(jnp.int32, (DQK, 128), 1)
    small_lane = lax.broadcasted_iota(jnp.int32, (TILE, 128), 1)
    small_row = lax.broadcasted_iota(jnp.int32, (TILE, 128), 0)
    biases = {0: [], 1: []}

    def pick_tables(t):
        for j in range(PICKS // 2):
            tiles, sides = [], []
            for e in range(2):
                pick = picks_ref[t, 2 * j + e]
                safe = jnp.where(pick < 0, 2 * i + t, pick)
                owner = safe // 2
                part = safe % 2
                ox, oz, oc = owner // 32, (owner // 2) % NZ, owner % 2
                tile = kb[oz, ox, pl.ds(pl.multiple_of(oc * DQK, 64), DQK), :].astype(F32)
                shift = part * 64 if e == 0 else (1 - part) * 64
                tiles.append(pltpu.roll(tile, shift, 1))
                start = pl.multiple_of(part * 64, 64)
                at = 128 * j + 64 * e
                vext[t, at:at + 64, :128] = vb[oz, ox, oc, pl.ds(start, 64), :]
                sides.append(jnp.where(pick < 0, LOW, 0.0).astype(F32))
            ks[t, 64:256, 128 * j:128 * j + 128] = jnp.where(
                half_lane < 64, tiles[0], tiles[1]
            ).astype(BF16)
            bias = jnp.where(small_lane < 64, sides[0], sides[1])
            if j == 0:
                bias = jnp.where((small_lane < 64) & (small_lane > small_row), LOW, bias)
            biases[t].append(bias)

    def queries_of(start, count, par):
        return jnp.concatenate(
            [
                q_vm[start:start + count, 384 * p + 128 * par:384 * p + 128 * par + 256]
                for p in range(PAIRS)
            ],
            0,
        )

    def scores(stage, buf):
        kind, par = stage
        if kind == 2:
            table = (even_sc, odd_sc)[par]
            s_sc[buf] = lax.dot_general(
                queries_of(0, ROWS, par), table[...], (((1,), (1,)), ((), ())),
                preferred_element_type=F32,
            )
        else:
            table = ks[kind, 64 - 64 * par:320 - 64 * par, :]
            s_sc[buf, :448, :] = jnp.dot(
                queries_of(64 * kind, 64, par), table, preferred_element_type=F32
            )

    def finish(stage, buf):
        kind, par = stage
        count = 2 * PAIRS if kind == 2 else PAIRS
        for p in range(count):
            rs = slice(64 * p, 64 * p + 64)
            if kind == 2:
                score = s_sc[buf, rs, :] + bias_sc[64 * (p % 2):64 * (p % 2) + 64, :]
            else:
                score = jnp.concatenate(
                    [
                        s_sc[buf, rs, 128 * j:128 * j + 128] + biases[kind][j]
                        for j in range(PICKS // 2)
                    ],
                    1,
                )
            top_score = jnp.maximum(jnp.max(score, axis=1, keepdims=True), FLOOR)
            p_sc[buf, rs, :] = jnp.exp2((score - top_score) * COEF).astype(BF16)
        result = jnp.dot(p_sc[buf, :64 * count, :], vext[kind], preferred_element_type=F32)
        for p in range(PAIRS):
            h = 2 * p + par
            if kind == 2:
                rs = slice(128 * p, 128 * p + 128)
                comp = result[rs, :128] / jnp.maximum(result[rs, 128:], 1.0)
                comp_sc[h] = gate_ref[:, 2 * h:2 * h + 1] * comp
            else:
                rs = slice(64 * kind, 64 * kind + 64)
                sel = result[64 * p:64 * p + 64, :128] / result[64 * p:64 * p + 64, 128:]
                mixed = comp_sc[h, rs] + gate_ref[rs, 2 * h + 1:2 * h + 2] * sel
                out_ref[rs, h * DV:(h + 1) * DV] = mixed.astype(BF16)

    stages = [(2, 0), (2, 1), (0, 0), (0, 1), (1, 0), (1, 1)]
    for n, stage in enumerate(stages):
        if n == 0:
            scores(stage, 0)
            pick_tables(0)
        if n + 1 < len(stages):
            scores(stages[n + 1], (n + 1) % 2)
        if n == 1:
            pick_tables(1)
        finish(stage, n % 2)


def local(queries, keys, values, key_weights, value_weights, picks, gates):
    vmem = pl.BlockSpec(memory_space=pltpu.VMEM)
    hbm = pl.BlockSpec(memory_space=pltpu.HBM)
    dma = pltpu.SemaphoreType.DMA
    kb, vb, rows, gate, listed = pl.pallas_call(
        gather_body,
        out_shape=[
            pltpu.VMEM((NZ, NX, KROWS, 128), BF16),
            pltpu.VMEM((NZ, NX, 2, ROWS, 128), BF16),
            pltpu.VMEM((ROWS, HEADS * DQK), BF16),
            pltpu.VMEM((ROWS, 32), F32),
            pltpu.SMEM((2, PICKS), jnp.int32),
        ],
        in_specs=[hbm] * 7,
        out_specs=[vmem] * 4 + [pl.BlockSpec(memory_space=pltpu.SMEM)],
        scratch_shapes=[
            pltpu.VMEM((32, DQK), F32),
            pltpu.VMEM((32, DV), F32),
            pltpu.VMEM((HEADS, 2, ROWS), F32),
            pltpu.VMEM((16, DQK), BF16),
            pltpu.VMEM((16, DQK), BF16),
            pltpu.VMEM((16, DV), BF16),
            dma((7,)),
            dma((2,)), dma((2,)),
            dma((2,)), dma((2,)),
            dma((2, 9, 3)), dma((2, 9, 3)),
            dma((2, 9, 4)), dma((2, 9, 4)),
            dma((3,)), dma((3,)),
            dma((NZ, 3, 2)), dma((NZ, 3, 2)),
            dma((NZ + 8,)), dma((NZ + 8,)),
            dma((NZ + 7,)), dma((NZ + 7,)),
        ],
        compiler_params=pltpu.CompilerParams(
            collective_id=0, has_side_effects=True, vmem_limit_bytes=50 * 1024 * 1024
        ),
        name="gather_rows",
    )(queries, keys.T, values, key_weights, value_weights, jnp.transpose(gates, (2, 0, 1)), picks)
    return pl.pallas_call(
        mix_body,
        out_shape=jax.ShapeDtypeStruct((ROWS, HEADS * DV), BF16),
        in_specs=[vmem] * 4 + [pl.BlockSpec(memory_space=pltpu.SMEM)],
        out_specs=vmem,
        scratch_shapes=[
            pltpu.VMEM((2, PAIRS * ROWS, 1024), F32),
            pltpu.VMEM((2, PAIRS * ROWS, 1024), BF16),
            pltpu.VMEM((2, 320, 1024), BF16),
            pltpu.VMEM((3, 1024, 256), BF16),
            pltpu.VMEM((1024, 256), BF16),
            pltpu.VMEM((1024, 256), BF16),
            pltpu.VMEM((ROWS, 1024), F32),
            pltpu.VMEM((HEADS, ROWS, 128), F32),
        ],
        compiler_params=pltpu.CompilerParams(vmem_limit_bytes=32 * 1024 * 1024),
        name="attend_mix",
    )(rows, kb, vb, gate, listed)


def solution(mesh):
    in_specs = (
        P("ctx", "kv"), P("ctx", "kv"), P("ctx", "kv"), P(None, "kv"), P(None, "kv"),
        P("ctx", None), P(None, "ctx", "kv"),
    )
    return jax.shard_map(
        local, mesh=mesh, in_specs=in_specs, out_specs=P("ctx", "kv"), check_vma=False
    )
```
